256 devices in a mesh: grp: 2 (over y), col: 32 (over z, core), blk: 4 (over x).
Axes of the slice: x: 4, y: 2, z: 16, core: 2. Of those that a mesh axis runs over, the one named last changes fastest.
The devices are a block of a 4x16x16 slice.
Arguments:
- boundary: bfloat16 [256, 192, 576], P(('grp', 'col'), 'blk'), parts along dimension 0, may hold values from -6 to 6
- row_tensor: bfloat16 [256, 6, 6, 6, 6], P(('grp', 'col')), parts along dimension 0, may hold values from -1.5 to 1.5
- left_proj: bfloat16 [256, 192, 576], P(('grp', 'col'), 'blk'), parts along dimension 0, may hold values from -0.75 to 0.75
- right_proj: bfloat16 [256, 192, 576], P(('grp', 'col'), 'blk'), parts along dimension 0, may hold values from -0.3125 to 0.3125
- leg_parity: int32 [256, 3, 6], P('grp'), parts along dimension 0, may hold values from 0 to 1
- bond_charges: int32 [256, 2], P('grp'), parts along dimension 0, may hold values from 32 to 96, as said below
Outputs:
- new_boundary: bfloat16 [256, 192, 576], P(('grp', 'col'), 'blk'), parts along dimension 0
The draws below stay inside these ranges and needn't reach their ends.
There are 2 independent parts, one for each index of `grp`. The reference program is written for one: setup_inputs(seed, part) draws one part's arguments, and reference() takes and returns one part's arrays. A program takes and returns all parts, laid end to end along the dimension named above; each array names one. Nothing has to cross between parts.
Inputs may be any that keep to these rules, and one draw needn't show every extreme that they name: `bond_charges`: odd counts are 128 minus these, so neither block of a bond holds more than 96 live rows; some bond has an even count of 96 and some bond an odd count of 96. `leg_parity`: [c, 0] is the horizontal leg left of column c, [c, 1] the vertical leg between boundary and row, [c, 2] the outgoing vertical leg.
All inputs are finite; a program needn't handle non-finite values.
Results may differ from the reference program's by a relative error of at most 0.0057.
Values may be sent and summed in bfloat16 or wider, within the bound.
A program may use at most 64 MiB of HBM per device.

```python
import jax
import jax.numpy as jnp
from jax import lax

CHI = 128
BLOCK = 96
D = 6
COLS = 128
PAD = 192


def draw_bond_charges(key, part):
    first_key, second_key, third_key = jax.random.split(jax.random.fold_in(key, 17), 3)
    counts = jax.random.randint(first_key, (COLS, 2), CHI - BLOCK, BLOCK + 1, dtype=jnp.int32)
    even_full = jax.random.randint(second_key, (), 0, COLS, dtype=jnp.int32)
    odd_full = jax.random.randint(third_key, (), 0, COLS, dtype=jnp.int32)
    counts = counts.at[even_full, 0].set(BLOCK)
    counts = counts.at[odd_full, 1].set(CHI - BLOCK)
    return counts


def plant(drawn, stream_key, least, largest):
    spot = [jax.random.randint(jax.random.fold_in(stream_key, axis), (), 0, length) for axis, length in enumerate(drawn.shape)]
    longest = drawn.shape.index(max(drawn.shape))
    neighbour = spot[:longest] + [(spot[longest] + 1) % drawn.shape[longest]] + spot[longest + 1:]
    return drawn.at[tuple(spot)].set(least).at[tuple(neighbour)].set(largest)


def level_of(key, extent, cuts, least, top_value):
    def one(axis_at, parts):
        heights = jax.random.uniform(jax.random.fold_in(jax.random.fold_in(key, 6), axis_at), (parts,), jnp.float32, least / len(cuts), top_value / len(cuts))
        return jnp.repeat(jnp.exp(heights), extent[axis_at] // parts).reshape((-1,) + (1,) * (len(extent) - axis_at - 1))

    loudness = one(*cuts[0])
    for cut in cuts[1:]:
        loudness = loudness * one(*cut)
    return loudness


def bell_draw(key, shape, spread, reach, pieces=(), kind=jnp.bfloat16):
    drawn = spread * jax.random.normal(key, shape, jnp.float32)
    if pieces:
        drawn = drawn * level_of(key, shape, pieces, -0.22, 0.18)
    return jnp.clip(drawn, -reach, reach).astype(kind)


def setup_inputs(seed: int = 0, part: int = 0) -> dict:
    arg_keys = jax.random.split(jax.random.key(seed), 7)
    part_keys = jax.random.split(jax.random.fold_in(arg_keys[6], part), 7)
    return {
        "boundary": bell_draw(part_keys[0], (COLS, PAD, D * BLOCK), 1.0, 6.0, ((0, 32), (1, 4))),
        "row_tensor": bell_draw(part_keys[1], (COLS, D, D, D, D), (D * D // 2) ** -0.5, 1.5, ((0, 32),)),
        "left_proj": bell_draw(part_keys[2], (COLS, PAD, D * BLOCK), (CHI // 2) ** -0.5, 0.75, ((0, 32), (1, 4))),
        "right_proj": bell_draw(part_keys[3], (COLS, PAD, D * BLOCK), (D * CHI // 2) ** -0.5, 0.3125, ((0, 32), (1, 4))),
        "leg_parity": plant(jax.random.randint(part_keys[4], (COLS, 3, D), 0, 2), jax.random.fold_in(part_keys[4], 1), 0, 1).astype(jnp.int32),
        "bond_charges": draw_bond_charges(jax.random.fold_in(jax.random.fold_in(arg_keys[6], part), 71), part),
    }


def live_rows(count, parity, position):
    limit = jnp.where(parity == 0, count, CHI - count)
    return (position < limit).astype(jnp.float32)


def reference(boundary, row_tensor, left_proj, right_proj, leg_parity, bond_charges):
    padded = 2 * BLOCK
    bound_all = boundary.reshape(COLS, padded, D, BLOCK)
    left_all = left_proj.reshape(COLS, padded, D, BLOCK)
    right_all = jnp.roll(right_proj.reshape(COLS, padded, D, BLOCK), -1, axis=0)
    charges_next = jnp.roll(bond_charges, -1, axis=0)
    legs_next = jnp.roll(leg_parity, -1, axis=0)
    indices = jnp.arange(padded, dtype=jnp.int32)
    parity_idx = indices // BLOCK
    position = indices % BLOCK
    inside = jnp.arange(BLOCK, dtype=jnp.int32)

    def column_step(inputs):
        bound_col, row_col, left_col, right_col, charge_here, charge_next, leg_here, leg_next = inputs
        left_leg = leg_here[0]
        up_leg = leg_here[1]
        down_leg = leg_here[2]
        right_leg = leg_next[0]
        bound_sel = (parity_idx[:, None] + up_leg[None, :]) % 2
        bound_mask = live_rows(charge_here[0], parity_idx, position)[:, None, None] * live_rows(
            charge_next[0], bound_sel[:, :, None], inside[None, None, :])
        bound_m = bound_col * bound_mask.astype(jnp.bfloat16)
        left_sel = (parity_idx[:, None] + left_leg[None, :]) % 2
        left_mask = live_rows(charge_here[1], parity_idx, position)[:, None, None] * live_rows(
            charge_here[0], left_sel[:, :, None], inside[None, None, :])
        left_m = left_col * left_mask.astype(jnp.bfloat16)
        left_dense = jnp.concatenate([
            left_m * (left_sel == 0).astype(jnp.bfloat16)[:, :, None],
            left_m * (left_sel == 1).astype(jnp.bfloat16)[:, :, None]], axis=2)
        right_sel = (parity_idx[:, None] + right_leg[None, :]) % 2
        right_mask = live_rows(charge_next[0], parity_idx, position)[:, None, None] * live_rows(
            charge_next[1], right_sel[:, :, None], inside[None, None, :])
        right_m = right_col * right_mask.astype(jnp.bfloat16)
        row_mask = ((left_leg[:, None, None, None] + up_leg[None, :, None, None]
                     + down_leg[None, None, :, None] + right_leg[None, None, None, :]) % 2 == 0).astype(jnp.float32)
        row_mask = row_mask * (1 - 2 * left_leg[:, None, None, None] * up_leg[None, :, None, None]).astype(jnp.float32)
        row_m = row_col * row_mask.astype(jnp.bfloat16)
        absorbed = jnp.dot(left_dense.reshape(padded * D, padded), bound_m.reshape(padded, D * BLOCK),
                           preferred_element_type=jnp.float32)
        absorbed = absorbed.astype(jnp.bfloat16).reshape(padded, D, D, BLOCK)
        mixed = jnp.einsum("plub,ludr->pdrb", absorbed.astype(jnp.float32), row_m.astype(jnp.float32))
        block_par = (parity_idx[:, None, None] + down_leg[None, :, None] + right_leg[None, None, :]) % 2
        sign_flip = (1 - 2 * block_par * down_leg[None, :, None]).astype(jnp.float32)
        mixed = (mixed * sign_flip[:, :, :, None]).astype(jnp.bfloat16)
        mixed_dense = jnp.concatenate([
            mixed * (block_par == 0).astype(jnp.bfloat16)[:, :, :, None],
            mixed * (block_par == 1).astype(jnp.bfloat16)[:, :, :, None]], axis=3)
        right_rb = jnp.transpose(right_m, (1, 0, 2)).reshape(D * padded, BLOCK)
        result = jnp.dot(mixed_dense.reshape(padded * D, D * padded), right_rb,
                         preferred_element_type=jnp.float32)
        return result.astype(jnp.bfloat16).reshape(padded, D * BLOCK)

    return lax.map(column_step, (bound_all, row_tensor, left_all, right_all,
                                 bond_charges, charges_next, leg_parity, legs_next))
```

```python
import functools

import jax
import jax.numpy as jnp
from jax import lax
from jax.experimental import pallas as pl
from jax.experimental.pallas import tpu as pltpu
from jax.sharding import PartitionSpec as P

CHI = 128
BLOCK = 96
D = 6
LANES = 128
SUB = 16
PAIRS = D * D
WIDE = PAIRS * SUB

MESH = pl.DeviceIdType.MESH
F32 = jnp.float32
BF16 = jnp.bfloat16


def ones_where(condition):
    return jnp.where(condition, 1.0, 0.0).astype(F32)


def iota(shape, dim):
    return lax.broadcasted_iota(jnp.int32, shape, dim)


def by_group(scalars, index, width):
    out = jnp.full(index.shape, scalars[0], jnp.int32)
    for i in range(1, len(scalars)):
        out = jnp.where(index >= i * width, scalars[i], out)
    return out


def limit_of(count, parity):
    return jnp.where(parity == 0, count, CHI - count)


def kernel(axis_sizes, bound_ref, left_ref, right_ref, row_ref, leg_ref, bond_ref, out_ref,
           bound_all, left_all, right_all, bound_x, left_x, right_x, mix, mid, dense, answer,
           send_sem, recv_sem, local_sem):
    n_col, n_blk = axis_sizes
    col_dev, sub_rows, merged = bound_ref.shape
    me = lax.axis_index("blk")
    col = lax.axis_index("col")
    last = n_blk - 1
    col_before = lax.rem(col + n_col - 1, n_col)
    col_after = lax.rem(col + 1, n_col)
    cols = bond_ref.shape[1]
    here = col * col_dev + me
    after = lax.rem(here + 1, cols)

    barrier = pltpu.get_barrier_semaphore()
    for k in range(1, n_blk):
        pl.semaphore_signal(barrier, inc=1, device_id={"blk": lax.rem(me + k, n_blk)}, device_id_type=MESH)

    @pl.when(me == last)
    def _():
        for t in range(n_blk):
            pl.semaphore_signal(barrier, inc=1, device_id={"col": col_after, "blk": t}, device_id_type=MESH)

    def rows(t):
        return pl.ds(pl.multiple_of(t * sub_rows, SUB), sub_rows)

    own_bound = pltpu.make_async_copy(bound_ref.at[me], bound_all.at[rows(me)], local_sem.at[0])
    own_left = pltpu.make_async_copy(left_ref.at[me], left_all.at[rows(me)], local_sem.at[1])
    own_bound.start()
    own_left.start()
    own_right = pltpu.make_async_copy(right_ref.at[lax.rem(me + 1, col_dev)], right_all.at[rows(me)], local_sem.at[2])

    @pl.when(me != last)
    def _():
        own_right.start()

    pl.semaphore_wait(barrier, n_blk)

    def sent(kind, k):
        t = lax.rem(me + k, n_blk)
        if kind == 0:
            source, target, where = bound_ref.at[t], bound_all, {"blk": t}
        elif kind == 1:
            source, target, where = left_ref.at[t], left_all, {"blk": t}
        else:
            c = jnp.where(t == last, col_before, col)
            source, target, where = right_ref.at[lax.rem(t + 1, col_dev)], right_all, {"col": c, "blk": t}
        return pltpu.make_async_remote_copy(
            src_ref=source, dst_ref=target.at[rows(me)],
            send_sem=send_sem.at[kind, k], recv_sem=recv_sem.at[kind, me],
            device_id=where, device_id_type=MESH)

    def arrived(kind, k):
        t = lax.rem(me + k, n_blk)
        source = (bound_ref, left_ref, right_ref)[kind]
        target = (bound_all, left_all, right_all)[kind]
        return pltpu.make_async_remote_copy(
            src_ref=source.at[0], dst_ref=target.at[rows(t)],
            send_sem=send_sem.at[kind, k], recv_sem=recv_sem.at[kind, t],
            device_id={"blk": t}, device_id_type=MESH)

    far_first = [2, 1, 3] if n_blk == 4 else list(range(1, n_blk))
    for kind in range(3):
        for k in far_first:
            sent(kind, k).start()

    @pl.when(me == last)
    def _():
        sent(2, 0).start()

    p0 = [leg_ref[0, i, here] for i in range(D)]
    p1 = [leg_ref[1, i, here] for i in range(D)]
    p2 = [leg_ref[2, i, here] for i in range(D)]
    pr = [leg_ref[0, i, after] for i in range(D)]
    in_here, out_here = bond_ref[0, here], bond_ref[1, here]
    in_next, out_next = bond_ref[0, after], bond_ref[1, after]

    triples = D * D * D
    pick = ones_where(iota((triples, triples * col_dev), 1) == iota((triples, triples * col_dev), 0) * col_dev + me)
    entries = jnp.dot(pick.astype(BF16), row_ref[...], preferred_element_type=F32).astype(BF16)
    lane = iota((D, LANES), 1)
    spread = ones_where((lane - iota((D, LANES), 0)) % D == 0)
    entries = jnp.dot(entries, spread.astype(BF16), preferred_element_type=F32)
    row = iota((triples, LANES), 0)
    lane = iota((triples, LANES), 1)
    d_row = row % D
    d_lane = lane // D
    legs_l = by_group(p0, row, D * D)
    legs_u = by_group(p1, (row // D) % D, 1)
    legs_d = by_group(p2, d_row, 1)
    legs_r = by_group(pr, lane % D, 1)
    total = legs_l + legs_u + legs_d + legs_r
    keep = (d_row == d_lane) & (total % 2 == 0)
    sign = 1 - 2 * legs_l * legs_u
    group = iota((WIDE, triples), 0) // SUB
    member = iota((WIDE, triples), 1)
    repeat = ones_where((member >= group * D) & (member < group * D + D)).astype(BF16)
    pair = ones_where(iota((WIDE, LANES), 0) // SUB == iota((WIDE, LANES), 1)).astype(BF16)
    same = ones_where(iota((WIDE, WIDE), 0) % SUB == iota((WIDE, WIDE), 1) % SUB)
    for p in range(2):
        q = (p + legs_d + legs_r) % 2
        signed = jnp.where(keep, sign * (1 - 2 * q * legs_d), 0).astype(F32)
        picked = (entries * signed).astype(BF16)
        stretched = jnp.dot(repeat, picked, preferred_element_type=F32).astype(BF16)
        full = lax.dot_general(pair, stretched, (((1,), (1,)), ((), ())), preferred_element_type=F32)
        mix[p] = (full * same).astype(BF16)

    zeros = jnp.zeros((2 * LANES - 2 * BLOCK, D * LANES), BF16)
    gap = LANES - BLOCK
    for p in range(2):
        bound_x[p * LANES + BLOCK:(p + 1) * LANES, :] = zeros[:gap]
    for r in range(D):
        right_x[r * LANES + BLOCK:(r + 1) * LANES, :] = zeros[:gap, :2 * LANES]
    lane_pad = jnp.zeros((sub_rows, gap), BF16)

    def widened(value, i):
        return jnp.concatenate([value[:, i * BLOCK:(i + 1) * BLOCK], lane_pad], axis=1)

    own_bound.wait()
    for k in far_first:
        arrived(0, k).wait_recv()
    for t in range(n_blk):
        p, half = t // 2, t % 2
        live = ones_where(half * sub_rows + iota((sub_rows, LANES), 0) < limit_of(in_here, p)).astype(BF16)
        value = bound_all[t * sub_rows:(t + 1) * sub_rows, :]
        for u in range(D):
            bound_x[p * LANES + half * sub_rows:p * LANES + (half + 1) * sub_rows,
                    u * LANES:(u + 1) * LANES] = widened(value, u) * live

    own_left.wait()
    for k in far_first:
        arrived(1, k).wait_recv()

    def right_ready():
        for k in far_first:
            arrived(2, k).wait_recv()

        @pl.when(me == last)
        def _():
            arrived(2, 0).wait_recv()

        @pl.when(me != last)
        def _():
            own_right.wait()

        for half in range(2):
            even = right_all[half * sub_rows:(half + 1) * sub_rows, :]
            odd = right_all[BLOCK + half * sub_rows:BLOCK + (half + 1) * sub_rows, :]
            position = half * sub_rows + iota((sub_rows, LANES), 0)
            even_live = ones_where(position < limit_of(in_next, 0)).astype(BF16)
            odd_live = ones_where(position < limit_of(in_next, 1)).astype(BF16)
            for r in range(D):
                a = widened(even, r) * even_live
                b = widened(odd, r) * odd_live
                at = slice(r * LANES + half * sub_rows, r * LANES + (half + 1) * sub_rows)
                right_x[at, :LANES] = jnp.where(pr[r] == 0, a, b)
                right_x[at, LANES:] = jnp.where(pr[r] == 0, b, a)

    own_half = me // 2
    groups = BLOCK // SUB
    for step in range(2):
        p = (own_half + 1 + step) % 2
        for half in range(2):
            value = left_all[pl.ds(pl.multiple_of(p * BLOCK + half * sub_rows, SUB), sub_rows), :]
            for leg in range(D):
                wide = widened(value, leg)
                at = slice(leg * BLOCK + half * sub_rows, leg * BLOCK + (half + 1) * sub_rows)
                odd = ((p + p0[leg]) % 2).astype(F32)
                left_x[at, :LANES] = wide * (1.0 - odd).astype(BF16)
                left_x[at, LANES:] = wide * odd.astype(BF16)
        for n in range(D // 2):
            part = jnp.dot(left_x[...], bound_x[:, n * 2 * LANES:(n + 1) * 2 * LANES],
                           preferred_element_type=F32).astype(BF16)
            for leg in range(D):
                for v in range(2):
                    at = (leg * D + 2 * n + v) * SUB
                    for g in range(groups):
                        mid[at:at + SUB, g * LANES:(g + 1) * LANES] = part[
                            leg * BLOCK + g * SUB:leg * BLOCK + (g + 1) * SUB, v * LANES:(v + 1) * LANES]
        for n in range(groups // 2):
            part = jnp.dot(mix[p], mid[:, n * 2 * LANES:(n + 1) * 2 * LANES],
                           preferred_element_type=F32).astype(BF16)
            for d in range(D):
                for r in range(D):
                    at = (d * D + r) * SUB
                    for v in range(2):
                        g = 2 * n + v
                        dense[d * BLOCK + g * SUB:d * BLOCK + (g + 1) * SUB, r * LANES:(r + 1) * LANES] = part[
                            at:at + SUB, v * LANES:(v + 1) * LANES]
        if step == 0:
            right_ready()
        position = iota((BLOCK, LANES), 0)
        row_live = position < limit_of(out_here, p)
        result = jnp.dot(dense[...], right_x[...], preferred_element_type=F32)
        for d in range(D):
            s = (p + p2[d]) % 2
            block = result[d * BLOCK:(d + 1) * BLOCK, :]
            chosen = jnp.where(s == 0, block[:, :LANES], block[:, LANES:])
            alive = row_live & (iota((BLOCK, LANES), 1) < limit_of(out_next, s))
            chosen = jnp.where(alive, chosen, 0.0).astype(BF16)[:, :BLOCK]
            for half in range(2):
                answer[2 * p + half, :, d * BLOCK:(d + 1) * BLOCK] = chosen[half * sub_rows:(half + 1) * sub_rows]
        for half in range(2):
            t = 2 * p + half

            @pl.when(t != me)
            def _():
                pltpu.make_async_remote_copy(
                    src_ref=answer.at[t], dst_ref=out_ref.at[me],
                    send_sem=send_sem.at[3, t], recv_sem=recv_sem.at[3, me],
                    device_id={"blk": t}, device_id_type=MESH).start()

            @pl.when(t == me)
            def _():
                pltpu.make_async_copy(answer.at[me], out_ref.at[me], local_sem.at[3]).start()

    pltpu.make_async_copy(answer.at[me], out_ref.at[me], local_sem.at[3]).wait()
    for k in far_first:
        t = lax.rem(me + k, n_blk)
        done = pltpu.make_async_remote_copy(
            src_ref=answer.at[t], dst_ref=out_ref.at[t],
            send_sem=send_sem.at[3, t], recv_sem=recv_sem.at[3, t],
            device_id={"blk": t}, device_id_type=MESH)
        done.wait_recv()
        done.wait_send()
        for kind in range(3):
            sent(kind, k).wait_send()

    @pl.when(me == last)
    def _():
        sent(2, 0).wait_send()


def per_device(axis_sizes, boundary, row_tensor, left_proj, right_proj, leg_parity, bond_charges):
    col_dev, sub_rows, merged = boundary.shape
    n_blk = axis_sizes[1]
    padded = n_blk * sub_rows
    rows = row_tensor.transpose(1, 2, 3, 0, 4).reshape(D * D * D * col_dev, D)
    anywhere = pl.BlockSpec(memory_space=pl.ANY)
    smem = pl.BlockSpec(memory_space=pltpu.SMEM)
    vmem = pl.BlockSpec(memory_space=pltpu.VMEM)
    return pl.pallas_call(
        functools.partial(kernel, axis_sizes),
        out_shape=jax.ShapeDtypeStruct(boundary.shape, BF16),
        in_specs=[anywhere, anywhere, anywhere, vmem, smem, smem],
        out_specs=vmem,
        scratch_shapes=[
            pltpu.VMEM((padded, merged), BF16),
            pltpu.VMEM((padded, merged), BF16),
            pltpu.VMEM((padded, merged), BF16),
            pltpu.VMEM((2 * LANES, D * LANES), BF16),
            pltpu.VMEM((D * BLOCK, 2 * LANES), BF16),
            pltpu.VMEM((D * LANES, 2 * LANES), BF16),
            pltpu.VMEM((2, WIDE, WIDE), BF16),
            pltpu.VMEM((WIDE, D * LANES), BF16),
            pltpu.VMEM((D * BLOCK, D * LANES), BF16),
            pltpu.VMEM((n_blk, sub_rows, merged), BF16),
            pltpu.SemaphoreType.DMA((4, n_blk)),
            pltpu.SemaphoreType.DMA((4, n_blk)),
            pltpu.SemaphoreType.DMA((4,)),
        ],
        compiler_params=pltpu.CompilerParams(collective_id=0, has_side_effects=True),
    )(boundary, left_proj, right_proj, rows, leg_parity.transpose(1, 2, 0), bond_charges.transpose(1, 0))


def solution(mesh):
    axis_sizes = (mesh.shape["col"], mesh.shape["blk"])
    in_specs = (
        P(("grp", "col"), "blk", None),
        P(("grp", "col"), None, None, None, None),
        P(("grp", "col"), "blk", None),
        P(("grp", "col"), "blk", None),
        P("grp", None, None),
        P("grp", None),
    )
    out_specs = P(("grp", "col"), "blk", None)
    return jax.shard_map(
        functools.partial(per_device, axis_sizes), mesh=mesh, in_specs=in_specs, out_specs=out_specs, check_vma=False
    )
```

```python
import functools

import jax
import jax.numpy as jnp
from jax import lax
from jax.experimental import pallas as pl
from jax.experimental.pallas import tpu as pltpu
from jax.sharding import PartitionSpec as P

CHI = 128
BLOCK = 96
D = 6
LANES = 128
SUB = 16
PAIRS = D * D
WIDE = PAIRS * SUB
VMEM_BYTES = 32 * 1024 * 1024

MESH = pl.DeviceIdType.MESH
F32 = jnp.float32
BF16 = jnp.bfloat16


def ones_where(condition):
    return jnp.where(condition, 1.0, 0.0).astype(F32)


def iota(shape, dim):
    return lax.broadcasted_iota(jnp.int32, shape, dim)


def by_group(scalars, index, width):
    out = jnp.full(index.shape, scalars[0], jnp.int32)
    for i in range(1, len(scalars)):
        out = jnp.where(index >= i * width, scalars[i], out)
    return out


def limit_of(count, parity):
    return jnp.where(parity == 0, count, CHI - count)


def kernel(axis_sizes, bound_ref, left_ref, right_ref, row_ref, leg_ref, bond_ref, out_ref,
           bound_all, left_all, left_shared, right_all, bound_x, left_x, right_x, mix, mid, dense, answer,
           send_sem, recv_sem, local_sem, ready_sem):
    n_col, n_blk = axis_sizes
    col_dev, sub_rows, merged = bound_ref.shape
    me = lax.axis_index("blk")
    col = lax.axis_index("col")
    last = n_blk - 1
    col_before = lax.rem(col + n_col - 1, n_col)
    col_after = lax.rem(col + 1, n_col)
    cols = bond_ref.shape[1]
    worker = me != 0

    barrier = pltpu.get_barrier_semaphore()
    pl.semaphore_signal(barrier, inc=1, device_id={"col": col_before, "blk": last}, device_id_type=MESH)

    @pl.when(worker)
    def _():
        for t in range(n_blk):
            @pl.when(me != t)
            def _():
                pl.semaphore_signal(barrier, inc=1, device_id={"blk": t}, device_id_type=MESH)

    def rows(t):
        return pl.ds(pl.multiple_of(t * sub_rows, SUB), sub_rows)

    targets = [bound_all.at[1], left_all, right_all.at[1], bound_all.at[0], right_all.at[0]]

    def source(kind, t):
        return (bound_ref.at[t], left_ref.at[t], right_ref.at[lax.rem(t + 1, col_dev)], bound_ref.at[0], right_ref.at[1])[kind]

    def own(kind):
        return pltpu.make_async_copy(source(kind, me), targets[kind].at[rows(me)], local_sem.at[kind])

    own(3).start()
    own(4).start()
    own_shared = pltpu.make_async_copy(left_ref.at[0], left_shared, local_sem.at[5])
    own_shared.start()

    @pl.when(worker)
    def _():
        own(0).start()
        own(1).start()

        @pl.when(me != last)
        def _():
            own(2).start()

    pl.semaphore_wait(barrier, jnp.where(me == 0, n_blk - 1, jnp.where(me == last, 2 * n_blk - 2, n_blk - 2)))

    def sent(kind, t):
        return pltpu.make_async_remote_copy(
            src_ref=source(kind, t), dst_ref=targets[kind].at[rows(me)],
            send_sem=send_sem.at[kind, t], recv_sem=recv_sem.at[kind, me],
            device_id={"blk": t}, device_id_type=MESH)

    def arrived(kind, t):
        return pltpu.make_async_remote_copy(
            src_ref=source(kind, 0), dst_ref=targets[kind].at[rows(t)],
            send_sem=send_sem.at[kind, t], recv_sem=recv_sem.at[kind, t],
            device_id={"blk": t}, device_id_type=MESH)

    beyond = pltpu.make_async_remote_copy(
        src_ref=right_ref.at[0], dst_ref=right_all.at[1, rows(me)],
        send_sem=send_sem.at[6, 0], recv_sem=recv_sem.at[2, me],
        device_id={"col": col_before, "blk": last}, device_id_type=MESH)

    @pl.when(me == 0)
    def _():
        for t in range(1, n_blk):
            pl.semaphore_signal(ready_sem.at[0], inc=1, device_id={"blk": t}, device_id_type=MESH)

    @pl.when(me == last)
    def _():
        for t in range(n_blk):
            pl.semaphore_signal(ready_sem.at[1], inc=1, device_id={"col": col_after, "blk": t}, device_id_type=MESH)

    kinds_to = {t: ([0, 2, 3, 4, 1] if t != last else [0, 3, 4, 1]) for t in range(1, n_blk)}
    for place in range(5):
        for t in (2, 1, 3):
            if place < len(kinds_to[t]):
                @pl.when(me != t)
                def _():
                    sent(kinds_to[t][place], t).start()

    triples = D * D * D
    group = iota((WIDE, triples), 0) // SUB
    member = iota((WIDE, triples), 1)
    repeat = ones_where((member >= group * D) & (member < group * D + D)).astype(BF16)
    pair = ones_where(iota((WIDE, LANES), 0) // SUB == iota((WIDE, LANES), 1)).astype(BF16)
    same = ones_where(iota((WIDE, WIDE), 0) % SUB == iota((WIDE, WIDE), 1) % SUB)
    spread = ones_where((iota((D, LANES), 1) - iota((D, LANES), 0)) % D == 0).astype(BF16)
    row = iota((triples, LANES), 0)
    lane = iota((triples, LANES), 1)
    d_row = row % D
    from_row = iota((triples, triples * col_dev), 0) * col_dev
    from_lane = iota((triples, triples * col_dev), 1)

    def legs_of(place):
        here = col * col_dev + place
        after = lax.rem(here + 1, cols)
        legs = [[leg_ref[i, j, here] for j in range(D)] for i in range(3)] + [[leg_ref[0, j, after] for j in range(D)]]
        return legs, (bond_ref[0, here], bond_ref[1, here], bond_ref[0, after], bond_ref[1, after])

    def build(place, legs, outputs):
        p0, p1, p2, pr = legs
        pick = ones_where(from_lane == from_row + place).astype(BF16)
        entries = jnp.dot(pick, row_ref[...], preferred_element_type=F32).astype(BF16)
        entries = jnp.dot(entries, spread, preferred_element_type=F32)
        legs_l = by_group(p0, row, D * D)
        legs_u = by_group(p1, (row // D) % D, 1)
        legs_d = by_group(p2, d_row, 1)
        legs_r = by_group(pr, lane % D, 1)
        keep = (d_row == lane // D) & ((legs_l + legs_u + legs_d + legs_r) % 2 == 0)
        sign = 1 - 2 * legs_l * legs_u
        for p, at in outputs:
            q = (p + legs_d + legs_r) % 2
            signed = jnp.where(keep, sign * (1 - 2 * q * legs_d), 0).astype(F32)
            stretched = jnp.dot(repeat, (entries * signed).astype(BF16), preferred_element_type=F32).astype(BF16)
            full = lax.dot_general(pair, stretched, (((1,), (1,)), ((), ())), preferred_element_type=F32)
            mix[at] = (full * same).astype(BF16)

    legs_shared, bonds_shared = legs_of(0)
    legs_mine, bonds_mine = legs_of(me)
    build(0, legs_shared, [(me // 2, 0)])

    @pl.when(worker)
    def _():
        build(me, legs_mine, [(0, 1), (1, 2)])

    gap = LANES - BLOCK
    lane_pad = jnp.zeros((sub_rows, gap), BF16)
    for slot in range(2):
        for p in range(2):
            bound_x[slot, p * LANES + BLOCK:(p + 1) * LANES, :] = jnp.zeros((gap, D * LANES), BF16)
        for r in range(D):
            right_x[slot, r * LANES + BLOCK:(r + 1) * LANES, :] = jnp.zeros((gap, 2 * LANES), BF16)

    @pl.when(worker)
    def _():
        pl.semaphore_wait(ready_sem.at[0], 1)
        sent(3, 0).start()
        sent(4, 0).start()

    def widened(value, i):
        return jnp.concatenate([value[:, i * BLOCK:(i + 1) * BLOCK], lane_pad], axis=1)

    def all_here(kind):
        for t in reversed(range(n_blk)):
            @pl.when(me != t)
            def _():
                arrived(kind, t).wait_recv()

            @pl.when(me == t)
            def _():
                if kind == 2 and t == last:
                    arrived(kind, t).wait_recv()
                else:
                    own(kind).wait()

    def boundary_ready(slot, bonds):
        all_here(0 if slot else 3)
        for t in range(n_blk):
            p, half = t // 2, t % 2
            live = ones_where(half * sub_rows + iota((sub_rows, LANES), 0) < limit_of(bonds[0], p)).astype(BF16)
            value = bound_all[slot, t * sub_rows:(t + 1) * sub_rows, :]
            at = p * LANES + half * sub_rows
            for u in range(D):
                bound_x[slot, at:at + sub_rows, u * LANES:(u + 1) * LANES] = widened(value, u) * live

    def right_ready(slot, legs, bonds):
        all_here(2 if slot else 4)
        pr = legs[3]
        for half in range(2):
            even = right_all[slot, half * sub_rows:(half + 1) * sub_rows, :]
            odd = right_all[slot, BLOCK + half * sub_rows:BLOCK + (half + 1) * sub_rows, :]
            position = half * sub_rows + iota((sub_rows, LANES), 0)
            even_live = ones_where(position < limit_of(bonds[2], 0)).astype(BF16)
            odd_live = ones_where(position < limit_of(bonds[2], 1)).astype(BF16)
            for r in range(D):
                a = widened(even, r) * even_live
                b = widened(odd, r) * odd_live
                at = slice(r * LANES + half * sub_rows, r * LANES + (half + 1) * sub_rows)
                right_x[slot, at, :LANES] = jnp.where(pr[r] == 0, a, b)
                right_x[slot, at, LANES:] = jnp.where(pr[r] == 0, b, a)

    groups = sub_rows // SUB

    def mixed_rows(slot, t, legs, value, buf):
        p = t // 2
        for leg in range(D):
            wide = widened(value, leg)
            odd = ((p + legs[0][leg]) % 2).astype(F32)
            left_x[buf, leg * sub_rows:(leg + 1) * sub_rows, :LANES] = wide * (1.0 - odd).astype(BF16)
            left_x[buf, leg * sub_rows:(leg + 1) * sub_rows, LANES:] = wide * odd.astype(BF16)
        for n in range(D // 2):
            part = jnp.dot(left_x[buf], bound_x[slot, :, n * 2 * LANES:(n + 1) * 2 * LANES],
                           preferred_element_type=F32).astype(BF16)
            for leg in range(D):
                for v in range(2):
                    at = (leg * D + 2 * n + v) * SUB
                    for g in range(groups):
                        mid[buf, at:at + SUB, g * LANES:(g + 1) * LANES] = part[
                            leg * sub_rows + g * SUB:leg * sub_rows + (g + 1) * SUB, v * LANES:(v + 1) * LANES]
        which = 0 if slot == 0 else 1 + p
        for lo in range(0, groups, 2):
            hi = min(lo + 2, groups)
            part = jnp.dot(mix[which], mid[buf, :, lo * LANES:hi * LANES], preferred_element_type=F32).astype(BF16)
            for d in range(D):
                for r in range(D):
                    at = (d * D + r) * SUB
                    for g in range(lo, hi):
                        dense[buf, d * sub_rows + g * SUB:d * sub_rows + (g + 1) * SUB, r * LANES:(r + 1) * LANES] = part[
                            at:at + SUB, (g - lo) * LANES:(g - lo + 1) * LANES]

    def new_rows(slot, t, legs, bonds, buf, target):
        p = t // 2
        position = (t % 2) * sub_rows + iota((sub_rows, LANES), 0)
        row_live = position < limit_of(bonds[1], p)
        result = jnp.dot(dense[buf], right_x[slot], preferred_element_type=F32)
        for d in range(D):
            s = (p + legs[2][d]) % 2
            block = result[d * sub_rows:(d + 1) * sub_rows, :]
            chosen = jnp.where(s == 0, block[:, :LANES], block[:, LANES:])
            alive = row_live & (iota((sub_rows, LANES), 1) < limit_of(bonds[3], s))
            target[:, d * BLOCK:(d + 1) * BLOCK] = jnp.where(alive, chosen, 0.0).astype(BF16)[:, :BLOCK]

    def returned(t):
        return pltpu.make_async_remote_copy(
            src_ref=answer.at[t], dst_ref=out_ref.at[me],
            send_sem=send_sem.at[5, t], recv_sem=recv_sem.at[5, me],
            device_id={"blk": t}, device_id_type=MESH)

    second = 1 + lax.rem(me, last)
    third = 1 + lax.rem(second, last)

    @pl.when(worker)
    def _():
        all_here(1)
        boundary_ready(1, bonds_mine)
        mixed_rows(1, second, legs_mine, left_all[rows(second), :], 0)

    pl.semaphore_wait(ready_sem.at[1], 1)
    beyond.start()

    @pl.when(worker)
    def _():
        right_ready(1, legs_mine, bonds_mine)
        new_rows(1, second, legs_mine, bonds_mine, 0, answer.at[second])
        returned(second).start()
        mixed_rows(1, third, legs_mine, left_all[rows(third), :], 1)
        new_rows(1, third, legs_mine, bonds_mine, 1, answer.at[third])
        returned(third).start()

    boundary_ready(0, bonds_shared)
    own_shared.wait()
    mixed_rows(0, me, legs_shared, left_shared[...], 0)
    right_ready(0, legs_shared, bonds_shared)
    new_rows(0, me, legs_shared, bonds_shared, 0, out_ref.at[0])

    @pl.when(worker)
    def _():
        mixed_rows(1, 0, legs_mine, left_all[rows(0), :], 1)
        new_rows(1, 0, legs_mine, bonds_mine, 1, answer.at[0])
        returned(0).start()
        mixed_rows(1, me, legs_mine, left_all[rows(me), :], 0)
        new_rows(1, me, legs_mine, bonds_mine, 0, out_ref.at[me])

    for t in range(1, n_blk):
        @pl.when(me != t)
        def _():
            pltpu.make_async_remote_copy(
                src_ref=answer.at[t], dst_ref=out_ref.at[t],
                send_sem=send_sem.at[5, t], recv_sem=recv_sem.at[5, t],
                device_id={"blk": t}, device_id_type=MESH).wait_recv()
            for kind in kinds_to[t]:
                sent(kind, t).wait_send()

    beyond.wait_send()

    @pl.when(worker)
    def _():
        sent(3, 0).wait_send()
        sent(4, 0).wait_send()
        returned(0).wait_send()
        returned(second).wait_send()
        returned(third).wait_send()


def per_device(axis_sizes, boundary, row_tensor, left_proj, right_proj, leg_parity, bond_charges):
    col_dev, sub_rows, merged = boundary.shape
    n_blk = axis_sizes[1]
    padded = n_blk * sub_rows
    rows = row_tensor.transpose(1, 2, 3, 0, 4).reshape(D * D * D * col_dev, D)
    anywhere = pl.BlockSpec(memory_space=pl.ANY)
    smem = pl.BlockSpec(memory_space=pltpu.SMEM)
    vmem = pl.BlockSpec(memory_space=pltpu.VMEM)
    return pl.pallas_call(
        functools.partial(kernel, axis_sizes),
        out_shape=jax.ShapeDtypeStruct(boundary.shape, BF16),
        in_specs=[anywhere, anywhere, anywhere, vmem, smem, smem],
        out_specs=vmem,
        scratch_shapes=[
            pltpu.VMEM((2, padded, merged), BF16),
            pltpu.VMEM((padded, merged), BF16),
            pltpu.VMEM((sub_rows, merged), BF16),
            pltpu.VMEM((2, padded, merged), BF16),
            pltpu.VMEM((2, 2 * LANES, D * LANES), BF16),
            pltpu.VMEM((2, D * sub_rows, 2 * LANES), BF16),
            pltpu.VMEM((2, D * LANES, 2 * LANES), BF16),
            pltpu.VMEM((3, WIDE, WIDE), BF16),
            pltpu.VMEM((2, WIDE, (sub_rows // SUB) * LANES), BF16),
            pltpu.VMEM((2, D * sub_rows, D * LANES), BF16),
            pltpu.VMEM((n_blk, sub_rows, merged), BF16),
            pltpu.SemaphoreType.DMA((7, n_blk)),
            pltpu.SemaphoreType.DMA((7, n_blk)),
            pltpu.SemaphoreType.DMA((6,)),
            pltpu.SemaphoreType.REGULAR((2,)),
        ],
        compiler_params=pltpu.CompilerParams(collective_id=0, has_side_effects=True, vmem_limit_bytes=VMEM_BYTES),
    )(boundary, left_proj, right_proj, rows, leg_parity.transpose(1, 2, 0), bond_charges.transpose(1, 0))


def solution(mesh):
    axis_sizes = (mesh.shape["col"], mesh.shape["blk"])
    in_specs = (
        P(("grp", "col"), "blk", None),
        P(("grp", "col"), None, None, None, None),
        P(("grp", "col"), "blk", None),
        P(("grp", "col"), "blk", None),
        P("grp", None, None),
        P("grp", None),
    )
    out_specs = P(("grp", "col"), "blk", None)
    return jax.shard_map(
        functools.partial(per_device, axis_sizes), mesh=mesh, in_specs=in_specs, out_specs=out_specs, check_vma=False
    )
```

```python
import functools

import jax
import jax.numpy as jnp
from jax import lax
from jax.experimental import pallas as pl
from jax.experimental.pallas import tpu as pltpu
from jax.sharding import PartitionSpec as P

CHI = 128
BLOCK = 96
D = 6
LANES = 128
SUB = 16
PAIRS = D * D
WIDE = PAIRS * SUB
VMEM_BYTES = 55 * 1024 * 1024

MESH = pl.DeviceIdType.MESH
F32 = jnp.float32
BF16 = jnp.bfloat16


def ones_where(condition):
    return jnp.where(condition, 1.0, 0.0).astype(F32)


def iota(shape, dim):
    return lax.broadcasted_iota(jnp.int32, shape, dim)


def by_group(scalars, index, width):
    out = jnp.full(index.shape, scalars[0], jnp.int32)
    for i in range(1, len(scalars)):
        out = jnp.where(index >= i * width, scalars[i], out)
    return out


def limit_of(count, parity):
    return jnp.where(parity == 0, count, CHI - count)


def kernel(axis_sizes, bound_ref, left_ref, right_ref, row_hbm, leg_hbm, bond_hbm, out_ref,
           row_ref, leg_ref, bond_ref, bound_all, left_all, left_shared, right_all, bound_x, left_x, right_x, mix, mid, dense, answer,
           send_sem, recv_sem, local_sem, ready_sem):
    n_col, n_blk = axis_sizes
    col_dev, sub_rows, merged = bound_ref.shape
    me = lax.axis_index("blk")
    col = lax.axis_index("col")
    last = n_blk - 1
    col_before = lax.rem(col + n_col - 1, n_col)
    col_after = lax.rem(col + 1, n_col)
    cols = bond_hbm.shape[1]
    worker = me != 0

    barrier = pltpu.get_barrier_semaphore()
    pl.semaphore_signal(barrier, inc=1, device_id={"col": col_before, "blk": last}, device_id_type=MESH)

    @pl.when(worker)
    def _():
        for t in range(n_blk):
            @pl.when(me != t)
            def _():
                pl.semaphore_signal(barrier, inc=1, device_id={"blk": t}, device_id_type=MESH)

    def rows(t):
        return pl.ds(pl.multiple_of(t * sub_rows, SUB), sub_rows)

    targets = [bound_all.at[1], left_all, right_all.at[1], bound_all.at[0], right_all.at[0]]

    def source(kind, t):
        return (bound_ref.at[t], left_ref.at[t], right_ref.at[lax.rem(t + 1, col_dev)], bound_ref.at[0], right_ref.at[1])[kind]

    def own(kind):
        return pltpu.make_async_copy(source(kind, me), targets[kind].at[rows(me)], local_sem.at[kind])

    small = [pltpu.make_async_copy(a, b, local_sem.at[6 + i])
             for i, (a, b) in enumerate([(row_hbm, row_ref), (leg_hbm, leg_ref), (bond_hbm, bond_ref)])]
    for copy in small:
        copy.start()
    own(3).start()
    own(4).start()
    own_shared = pltpu.make_async_copy(left_ref.at[0], left_shared, local_sem.at[5])
    own_shared.start()

    @pl.when(worker)
    def _():
        own(0).start()
        own(1).start()

        @pl.when(me != last)
        def _():
            own(2).start()

    pl.semaphore_wait(barrier, jnp.where(me == 0, n_blk - 1, jnp.where(me == last, 2 * n_blk - 2, n_blk - 2)))

    def sent(kind, t):
        return pltpu.make_async_remote_copy(
            src_ref=source(kind, t), dst_ref=targets[kind].at[rows(me)],
            send_sem=send_sem.at[kind, t], recv_sem=recv_sem.at[kind, me],
            device_id={"blk": t}, device_id_type=MESH)

    def arrived(kind, t):
        return pltpu.make_async_remote_copy(
            src_ref=source(kind, 0), dst_ref=targets[kind].at[rows(t)],
            send_sem=send_sem.at[kind, t], recv_sem=recv_sem.at[kind, t],
            device_id={"blk": t}, device_id_type=MESH)

    beyond = pltpu.make_async_remote_copy(
        src_ref=right_ref.at[0], dst_ref=right_all.at[1, rows(me)],
        send_sem=send_sem.at[6, 0], recv_sem=recv_sem.at[2, me],
        device_id={"col": col_before, "blk": last}, device_id_type=MESH)

    @pl.when(me == 0)
    def _():
        for t in range(1, n_blk):
            pl.semaphore_signal(ready_sem.at[0], inc=1, device_id={"blk": t}, device_id_type=MESH)

    @pl.when(me == last)
    def _():
        for t in range(n_blk):
            pl.semaphore_signal(ready_sem.at[1], inc=1, device_id={"col": col_after, "blk": t}, device_id_type=MESH)

    kinds_to = {t: ([0, 2, 3, 4, 1] if t != last else [0, 3, 4, 1]) for t in range(1, n_blk)}
    for place in range(5):
        for t in (2, 1, 3):
            if place < len(kinds_to[t]):
                @pl.when(me != t)
                def _():
                    sent(kinds_to[t][place], t).start()

    for copy in small:
        copy.wait()

    triples = D * D * D
    group = iota((WIDE, triples), 0) // SUB
    member = iota((WIDE, triples), 1)
    repeat = ones_where((member >= group * D) & (member < group * D + D)).astype(BF16)
    pair = ones_where(iota((WIDE, LANES), 0) // SUB == iota((WIDE, LANES), 1)).astype(BF16)
    same = ones_where(iota((WIDE, WIDE), 0) % SUB == iota((WIDE, WIDE), 1) % SUB)
    spread = ones_where((iota((D, LANES), 1) - iota((D, LANES), 0)) % D == 0).astype(BF16)
    row = iota((triples, LANES), 0)
    lane = iota((triples, LANES), 1)
    d_row = row % D
    from_row = iota((triples, triples * col_dev), 0) * col_dev
    from_lane = iota((triples, triples * col_dev), 1)

    def legs_of(place):
        here = col * col_dev + place
        after = lax.rem(here + 1, cols)
        legs = [[leg_ref[i, j, here] for j in range(D)] for i in range(3)] + [[leg_ref[0, j, after] for j in range(D)]]
        return legs, (bond_ref[0, here], bond_ref[1, here], bond_ref[0, after], bond_ref[1, after])

    def build(place, legs, outputs):
        p0, p1, p2, pr = legs
        pick = ones_where(from_lane == from_row + place).astype(BF16)
        entries = jnp.dot(pick, row_ref[...], preferred_element_type=F32).astype(BF16)
        entries = jnp.dot(entries, spread, preferred_element_type=F32)
        legs_l = by_group(p0, row, D * D)
        legs_u = by_group(p1, (row // D) % D, 1)
        legs_d = by_group(p2, d_row, 1)
        legs_r = by_group(pr, lane % D, 1)
        keep = (d_row == lane // D) & ((legs_l + legs_u + legs_d + legs_r) % 2 == 0)
        sign = 1 - 2 * legs_l * legs_u
        for p, at in outputs:
            q = (p + legs_d + legs_r) % 2
            signed = jnp.where(keep, sign * (1 - 2 * q * legs_d), 0).astype(F32)
            stretched = jnp.dot(repeat, (entries * signed).astype(BF16), preferred_element_type=F32).astype(BF16)
            full = lax.dot_general(pair, stretched, (((1,), (1,)), ((), ())), preferred_element_type=F32)
            mix[at] = (full * same).astype(BF16)

    legs_shared, bonds_shared = legs_of(0)
    legs_mine, bonds_mine = legs_of(me)
    build(0, legs_shared, [(me // 2, 0)])

    @pl.when(worker)
    def _():
        build(me, legs_mine, [(0, 1), (1, 2)])

    gap = LANES - BLOCK
    lane_pad = jnp.zeros((sub_rows, gap), BF16)
    for slot in range(2):
        for p in range(2):
            bound_x[slot, p * LANES + BLOCK:(p + 1) * LANES, :] = jnp.zeros((gap, D * LANES), BF16)
        for r in range(D):
            right_x[slot, r * LANES + BLOCK:(r + 1) * LANES, :] = jnp.zeros((gap, 2 * LANES), BF16)

    @pl.when(worker)
    def _():
        pl.semaphore_wait(ready_sem.at[0], 1)
        sent(3, 0).start()
        sent(4, 0).start()

    def pass_beyond():
        pl.semaphore_wait(ready_sem.at[1], 1)
        beyond.start()

    @pl.when(col != 0)
    def _():
        pass_beyond()

    def widened(value, i):
        return jnp.concatenate([value[:, i * BLOCK:(i + 1) * BLOCK], lane_pad], axis=1)

    def here(kind, t):
        @pl.when(me != t)
        def _():
            arrived(kind, t).wait_recv()

        @pl.when(me == t)
        def _():
            if kind == 2 and t == last:
                arrived(kind, t).wait_recv()
            else:
                own(kind).wait()

    def boundary_ready(slot, bonds):
        for t in reversed(range(n_blk)):
            here(0 if slot else 3, t)
            p, half = t // 2, t % 2
            live = ones_where(half * sub_rows + iota((sub_rows, LANES), 0) < limit_of(bonds[0], p)).astype(BF16)
            value = bound_all[slot, t * sub_rows:(t + 1) * sub_rows, :]
            at = p * LANES + half * sub_rows
            for u in range(D):
                bound_x[slot, at:at + sub_rows, u * LANES:(u + 1) * LANES] = widened(value, u) * live

    def right_ready(slot, legs, bonds):
        pr = legs[3]
        for t in reversed(range(n_blk)):
            here(2 if slot else 4, t)
            p, half = t // 2, t % 2
            position = half * sub_rows + iota((sub_rows, LANES), 0)
            live = ones_where(position < limit_of(bonds[2], p)).astype(BF16)
            value = right_all[slot, t * sub_rows:(t + 1) * sub_rows, :]
            for r in range(D):
                wide = widened(value, r) * live
                at = slice(r * LANES + half * sub_rows, r * LANES + (half + 1) * sub_rows)

                if p == 1:
                    right_x[slot, at, :LANES] = wide
                    right_x[slot, at, LANES:] = wide
                else:
                    right_x[slot, at, :LANES] = jnp.where(pr[r] == 0, wide, right_x[slot, at, :LANES])
                    right_x[slot, at, LANES:] = jnp.where(pr[r] == 0, right_x[slot, at, LANES:], wide)

    groups = sub_rows // SUB

    def mixed_rows(slot, t, legs, value, buf):
        p = t // 2
        for leg in range(D):
            wide = widened(value, leg)
            odd = ((p + legs[0][leg]) % 2).astype(F32)
            left_x[buf, leg * sub_rows:(leg + 1) * sub_rows, :LANES] = wide * (1.0 - odd).astype(BF16)
            left_x[buf, leg * sub_rows:(leg + 1) * sub_rows, LANES:] = wide * odd.astype(BF16)
        for n in range(D // 2):
            part = jnp.dot(left_x[buf], bound_x[slot, :, n * 2 * LANES:(n + 1) * 2 * LANES],
                           preferred_element_type=F32).astype(BF16)
            for leg in range(D):
                for v in range(2):
                    at = (leg * D + 2 * n + v) * SUB
                    for g in range(groups):
                        mid[buf, at:at + SUB, g * LANES:(g + 1) * LANES] = part[
                            leg * sub_rows + g * SUB:leg * sub_rows + (g + 1) * SUB, v * LANES:(v + 1) * LANES]
        which = 0 if slot == 0 else 1 + p
        for lo in range(0, groups, 2):
            hi = min(lo + 2, groups)
            part = jnp.dot(mix[which], mid[buf, :, lo * LANES:hi * LANES], preferred_element_type=F32).astype(BF16)
            for d in range(D):
                for r in range(D):
                    at = (d * D + r) * SUB
                    for g in range(lo, hi):
                        dense[buf, d * sub_rows + g * SUB:d * sub_rows + (g + 1) * SUB, r * LANES:(r + 1) * LANES] = part[
                            at:at + SUB, (g - lo) * LANES:(g - lo + 1) * LANES]

    def new_rows(slot, t, legs, bonds, buf, target):
        p = t // 2
        position = (t % 2) * sub_rows + iota((sub_rows, LANES), 0)
        row_live = position < limit_of(bonds[1], p)
        result = jnp.dot(dense[buf], right_x[slot], preferred_element_type=F32)
        for d in range(D):
            s = (p + legs[2][d]) % 2
            block = result[d * sub_rows:(d + 1) * sub_rows, :]
            chosen = jnp.where(s == 0, block[:, :LANES], block[:, LANES:])
            alive = row_live & (iota((sub_rows, LANES), 1) < limit_of(bonds[3], s))
            target[:, d * BLOCK:(d + 1) * BLOCK] = jnp.where(alive, chosen, 0.0).astype(BF16)[:, :BLOCK]

    def returned(t):
        return pltpu.make_async_remote_copy(
            src_ref=answer.at[t], dst_ref=out_ref.at[me],
            send_sem=send_sem.at[5, t], recv_sem=recv_sem.at[5, me],
            device_id={"blk": t}, device_id_type=MESH)

    second = 1 + lax.rem(me, last)
    third = 1 + lax.rem(second, last)

    @pl.when(worker)
    def _():
        for t in range(1, n_blk):
            here(1, t)
        boundary_ready(1, bonds_mine)
        mixed_rows(1, second, legs_mine, left_all[rows(second), :], 0)

        right_ready(1, legs_mine, bonds_mine)
        new_rows(1, second, legs_mine, bonds_mine, 0, answer.at[second])
        returned(second).start()
        mixed_rows(1, third, legs_mine, left_all[rows(third), :], 1)
        new_rows(1, third, legs_mine, bonds_mine, 1, answer.at[third])
        returned(third).start()

    boundary_ready(0, bonds_shared)
    own_shared.wait()
    mixed_rows(0, me, legs_shared, left_shared[...], 0)
    right_ready(0, legs_shared, bonds_shared)
    new_rows(0, me, legs_shared, bonds_shared, 0, out_ref.at[0])

    @pl.when(worker)
    def _():
        here(1, 0)
        mixed_rows(1, 0, legs_mine, left_all[rows(0), :], 1)
        new_rows(1, 0, legs_mine, bonds_mine, 1, answer.at[0])
        returned(0).start()
        mixed_rows(1, me, legs_mine, left_all[rows(me), :], 0)
        new_rows(1, me, legs_mine, bonds_mine, 0, out_ref.at[me])

    @pl.when(col == 0)
    def _():
        pass_beyond()

    for t in range(1, n_blk):
        @pl.when(me != t)
        def _():
            pltpu.make_async_remote_copy(
                src_ref=answer.at[t], dst_ref=out_ref.at[t],
                send_sem=send_sem.at[5, t], recv_sem=recv_sem.at[5, t],
                device_id={"blk": t}, device_id_type=MESH).wait_recv()
            for kind in kinds_to[t]:
                sent(kind, t).wait_send()

    beyond.wait_send()

    @pl.when(worker)
    def _():
        sent(3, 0).wait_send()
        sent(4, 0).wait_send()
        returned(0).wait_send()
        returned(second).wait_send()
        returned(third).wait_send()


def per_device(axis_sizes, boundary, row_tensor, left_proj, right_proj, leg_parity, bond_charges):
    col_dev, sub_rows, merged = boundary.shape
    n_blk = axis_sizes[1]
    padded = n_blk * sub_rows
    legs = leg_parity.transpose(1, 2, 0)
    bonds = bond_charges.transpose(1, 0)
    rows = row_tensor.transpose(1, 2, 3, 0, 4).reshape(D * D * D * col_dev, D)
    hbm = pl.BlockSpec(memory_space=pltpu.HBM)
    vmem = pl.BlockSpec(memory_space=pltpu.VMEM)
    return pl.pallas_call(
        functools.partial(kernel, axis_sizes),
        out_shape=pltpu.VMEM(boundary.shape, BF16),
        in_specs=[hbm] * 6,
        out_specs=vmem,
        scratch_shapes=[
            pltpu.VMEM(rows.shape, BF16),
            pltpu.SMEM(legs.shape, jnp.int32),
            pltpu.SMEM(bonds.shape, jnp.int32),
            pltpu.VMEM((2, padded, merged), BF16),
            pltpu.VMEM((padded, merged), BF16),
            pltpu.VMEM((sub_rows, merged), BF16),
            pltpu.VMEM((2, padded, merged), BF16),
            pltpu.VMEM((2, 2 * LANES, D * LANES), BF16),
            pltpu.VMEM((2, D * sub_rows, 2 * LANES), BF16),
            pltpu.VMEM((2, D * LANES, 2 * LANES), BF16),
            pltpu.VMEM((3, WIDE, WIDE), BF16),
            pltpu.VMEM((2, WIDE, (sub_rows // SUB) * LANES), BF16),
            pltpu.VMEM((2, D * sub_rows, D * LANES), BF16),
            pltpu.VMEM((n_blk, sub_rows, merged), BF16),
            pltpu.SemaphoreType.DMA((7, n_blk)),
            pltpu.SemaphoreType.DMA((7, n_blk)),
            pltpu.SemaphoreType.DMA((9,)),
            pltpu.SemaphoreType.REGULAR((2,)),
        ],
        compiler_params=pltpu.CompilerParams(collective_id=0, has_side_effects=True, vmem_limit_bytes=VMEM_BYTES),
    )(boundary, left_proj, right_proj, rows, legs, bonds)


def solution(mesh):
    axis_sizes = (mesh.shape["col"], mesh.shape["blk"])
    in_specs = (
        P(("grp", "col"), "blk", None),
        P(("grp", "col"), None, None, None, None),
        P(("grp", "col"), "blk", None),
        P(("grp", "col"), "blk", None),
        P("grp", None, None),
        P("grp", None),
    )
    out_specs = P(("grp", "col"), "blk", None)
    return jax.shard_map(
        functools.partial(per_device, axis_sizes), mesh=mesh, in_specs=in_specs, out_specs=out_specs, check_vma=False
    )
```

```python
import functools

import jax
import jax.numpy as jnp
from jax import lax
from jax.experimental import pallas as pl
from jax.experimental.pallas import tpu as pltpu
from jax.sharding import PartitionSpec as P

CHI = 128
BLOCK = 96
D = 6
LANES = 128
SUB = 16
PAIRS = D * D
WIDE = PAIRS * SUB
VMEM_BYTES = 55 * 1024 * 1024

MESH = pl.DeviceIdType.MESH
F32 = jnp.float32
BF16 = jnp.bfloat16


def ones_where(condition):
    return jnp.where(condition, 1.0, 0.0).astype(F32)


def iota(shape, dim):
    return lax.broadcasted_iota(jnp.int32, shape, dim)


def by_group(scalars, index, width):
    out = jnp.full(index.shape, scalars[0], jnp.int32)
    for i in range(1, len(scalars)):
        out = jnp.where(index >= i * width, scalars[i], out)
    return out


def limit_of(count, parity):
    return jnp.where(parity == 0, count, CHI - count)


def kernel(axis_sizes, bound_ref, left_ref, right_ref, row_hbm, leg_hbm, bond_hbm, out_ref,
           row_ref, leg_ref, bond_ref, bound_all, left_all, left_shared, right_all, bound_x, left_x, right_x, mix, mid, dense, answer,
           send_sem, recv_sem, local_sem, ready_sem):
    n_col, n_blk = axis_sizes
    col_dev, sub_rows, merged = bound_ref.shape
    me = lax.axis_index("blk")
    col = lax.axis_index("col")
    last = n_blk - 1
    col_before = lax.rem(col + n_col - 1, n_col)
    col_after = lax.rem(col + 1, n_col)
    cols = bond_hbm.shape[1]
    worker = me != 0

    barrier = pltpu.get_barrier_semaphore()
    pl.semaphore_signal(barrier, inc=1, device_id={"col": col_before, "blk": last}, device_id_type=MESH)

    @pl.when(worker)
    def _():
        for t in range(n_blk):
            @pl.when(me != t)
            def _():
                pl.semaphore_signal(barrier, inc=1, device_id={"blk": t}, device_id_type=MESH)

    def rows(t):
        return pl.ds(pl.multiple_of(t * sub_rows, SUB), sub_rows)

    targets = [bound_all.at[1], left_all, right_all.at[1], bound_all.at[0], right_all.at[0]]

    def source(kind, t):
        return (bound_ref.at[t], left_ref.at[t], right_ref.at[lax.rem(t + 1, col_dev)], bound_ref.at[0], right_ref.at[1])[kind]

    def own(kind):
        return pltpu.make_async_copy(source(kind, me), targets[kind].at[rows(me)], local_sem.at[kind])

    small = [pltpu.make_async_copy(a, b, local_sem.at[6 + i])
             for i, (a, b) in enumerate([(row_hbm, row_ref), (leg_hbm, leg_ref), (bond_hbm, bond_ref)])]
    for copy in small:
        copy.start()
    own(3).start()
    own(4).start()
    own_shared = pltpu.make_async_copy(left_ref.at[0], left_shared, local_sem.at[5])
    own_shared.start()

    @pl.when(worker)
    def _():
        own(0).start()
        own(1).start()

        @pl.when(me != last)
        def _():
            own(2).start()

    pl.semaphore_wait(barrier, jnp.where(me == 0, n_blk - 1, jnp.where(me == last, 2 * n_blk - 2, n_blk - 2)))

    def sent(kind, t):
        return pltpu.make_async_remote_copy(
            src_ref=source(kind, t), dst_ref=targets[kind].at[rows(me)],
            send_sem=send_sem.at[kind, t], recv_sem=recv_sem.at[kind, me],
            device_id={"blk": t}, device_id_type=MESH)

    def arrived(kind, t):
        return pltpu.make_async_remote_copy(
            src_ref=source(kind, 0), dst_ref=targets[kind].at[rows(t)],
            send_sem=send_sem.at[kind, t], recv_sem=recv_sem.at[kind, t],
            device_id={"blk": t}, device_id_type=MESH)

    beyond = pltpu.make_async_remote_copy(
        src_ref=right_ref.at[0], dst_ref=right_all.at[1, rows(me)],
        send_sem=send_sem.at[6, 0], recv_sem=recv_sem.at[2, me],
        device_id={"col": col_before, "blk": last}, device_id_type=MESH)

    @pl.when(me == 0)
    def _():
        for t in range(1, n_blk):
            pl.semaphore_signal(ready_sem.at[0], inc=1, device_id={"blk": t}, device_id_type=MESH)

    @pl.when(me == last)
    def _():
        for t in range(n_blk):
            pl.semaphore_signal(ready_sem.at[1], inc=1, device_id={"col": col_after, "blk": t}, device_id_type=MESH)

    kinds_to = {t: ([0, 1, 2, 3, 4] if t != last else [0, 1, 3, 4]) for t in range(1, n_blk)}

    @pl.when(me == 0)
    def _():
        for kind in (0, 2, 1, 3, 4):
            for t in (2, 1, 3):
                if kind in kinds_to[t]:
                    sent(kind, t).start()

    @pl.when(worker)
    def _():
        for kind in (0, 1, 2, 3, 4):
            for t in (2, 1, 3):
                if kind in kinds_to[t]:
                    @pl.when(me != t)
                    def _():
                        sent(kind, t).start()

    for copy in small:
        copy.wait()

    triples = D * D * D
    group = iota((WIDE, triples), 0) // SUB
    member = iota((WIDE, triples), 1)
    repeat = ones_where((member >= group * D) & (member < group * D + D)).astype(BF16)
    pair = ones_where(iota((WIDE, LANES), 0) // SUB == iota((WIDE, LANES), 1)).astype(BF16)
    same = ones_where(iota((WIDE, WIDE), 0) % SUB == iota((WIDE, WIDE), 1) % SUB)
    spread = ones_where((iota((D, LANES), 1) - iota((D, LANES), 0)) % D == 0).astype(BF16)
    row = iota((triples, LANES), 0)
    lane = iota((triples, LANES), 1)
    d_row = row % D
    from_row = iota((triples, triples * col_dev), 0) * col_dev
    from_lane = iota((triples, triples * col_dev), 1)

    def legs_of(place):
        here = col * col_dev + place
        after = lax.rem(here + 1, cols)
        legs = [[leg_ref[i, j, here] for j in range(D)] for i in range(3)] + [[leg_ref[0, j, after] for j in range(D)]]
        return legs, (bond_ref[0, here], bond_ref[1, here], bond_ref[0, after], bond_ref[1, after])

    def build(place, legs, outputs):
        p0, p1, p2, pr = legs
        pick = ones_where(from_lane == from_row + place).astype(BF16)
        entries = jnp.dot(pick, row_ref[...], preferred_element_type=F32).astype(BF16)
        entries = jnp.dot(entries, spread, preferred_element_type=F32)
        legs_l = by_group(p0, row, D * D)
        legs_u = by_group(p1, (row // D) % D, 1)
        legs_d = by_group(p2, d_row, 1)
        legs_r = by_group(pr, lane % D, 1)
        keep = (d_row == lane // D) & ((legs_l + legs_u + legs_d + legs_r) % 2 == 0)
        sign = 1 - 2 * legs_l * legs_u
        for p, at in outputs:
            q = (p + legs_d + legs_r) % 2
            signed = jnp.where(keep, sign * (1 - 2 * q * legs_d), 0).astype(F32)
            stretched = jnp.dot(repeat, (entries * signed).astype(BF16), preferred_element_type=F32).astype(BF16)
            full = lax.dot_general(pair, stretched, (((1,), (1,)), ((), ())), preferred_element_type=F32)
            mix[at] = (full * same).astype(BF16)

    legs_shared, bonds_shared = legs_of(0)
    legs_mine, bonds_mine = legs_of(me)
    build(0, legs_shared, [(me // 2, 0)])

    @pl.when(worker)
    def _():
        build(me, legs_mine, [(0, 1), (1, 2)])

    gap = LANES - BLOCK
    lane_pad = jnp.zeros((sub_rows, gap), BF16)
    for slot in range(2):
        for p in range(2):
            bound_x[slot, p * LANES + BLOCK:(p + 1) * LANES, :] = jnp.zeros((gap, D * LANES), BF16)
        for r in range(D):
            right_x[slot, r * LANES + BLOCK:(r + 1) * LANES, :] = jnp.zeros((gap, 2 * LANES), BF16)

    @pl.when(worker)
    def _():
        pl.semaphore_wait(ready_sem.at[0], 1)
        sent(3, 0).start()
        sent(4, 0).start()

    def pass_beyond():
        pl.semaphore_wait(ready_sem.at[1], 1)
        beyond.start()

    @pl.when(col != 0)
    def _():
        pass_beyond()

    def widened(value, i):
        return jnp.concatenate([value[:, i * BLOCK:(i + 1) * BLOCK], lane_pad], axis=1)

    def here(kind, t):
        @pl.when(me != t)
        def _():
            arrived(kind, t).wait_recv()

        @pl.when(me == t)
        def _():
            if kind == 2 and t == last:
                arrived(kind, t).wait_recv()
            else:
                own(kind).wait()

    def boundary_ready(slot, bonds):
        for t in reversed(range(n_blk)):
            here(0 if slot else 3, t)
            p, half = t // 2, t % 2
            live = ones_where(half * sub_rows + iota((sub_rows, LANES), 0) < limit_of(bonds[0], p)).astype(BF16)
            value = bound_all[slot, t * sub_rows:(t + 1) * sub_rows, :]
            at = p * LANES + half * sub_rows
            for u in range(D):
                bound_x[slot, at:at + sub_rows, u * LANES:(u + 1) * LANES] = widened(value, u) * live

    def right_ready(slot, legs, bonds):
        pr = legs[3]
        for t in reversed(range(n_blk)):
            here(2 if slot else 4, t)
            p, half = t // 2, t % 2
            position = half * sub_rows + iota((sub_rows, LANES), 0)
            live = ones_where(position < limit_of(bonds[2], p)).astype(BF16)
            value = right_all[slot, t * sub_rows:(t + 1) * sub_rows, :]
            for r in range(D):
                wide = widened(value, r) * live
                at = slice(r * LANES + half * sub_rows, r * LANES + (half + 1) * sub_rows)

                if p == 1:
                    right_x[slot, at, :LANES] = wide
                    right_x[slot, at, LANES:] = wide
                else:
                    right_x[slot, at, :LANES] = jnp.where(pr[r] == 0, wide, right_x[slot, at, :LANES])
                    right_x[slot, at, LANES:] = jnp.where(pr[r] == 0, right_x[slot, at, LANES:], wide)

    groups = sub_rows // SUB

    def mixed_rows(slot, t, legs, value, buf):
        p = t // 2
        for leg in range(D):
            wide = widened(value, leg)
            odd = ((p + legs[0][leg]) % 2).astype(F32)
            left_x[buf, leg * sub_rows:(leg + 1) * sub_rows, :LANES] = wide * (1.0 - odd).astype(BF16)
            left_x[buf, leg * sub_rows:(leg + 1) * sub_rows, LANES:] = wide * odd.astype(BF16)
        for n in range(D // 2):
            part = jnp.dot(left_x[buf], bound_x[slot, :, n * 2 * LANES:(n + 1) * 2 * LANES],
                           preferred_element_type=F32).astype(BF16)
            for leg in range(D):
                for v in range(2):
                    at = (leg * D + 2 * n + v) * SUB
                    for g in range(groups):
                        mid[buf, at:at + SUB, g * LANES:(g + 1) * LANES] = part[
                            leg * sub_rows + g * SUB:leg * sub_rows + (g + 1) * SUB, v * LANES:(v + 1) * LANES]
        which = 0 if slot == 0 else 1 + p
        for lo in range(0, groups, 2):
            hi = min(lo + 2, groups)
            part = jnp.dot(mix[which], mid[buf, :, lo * LANES:hi * LANES], preferred_element_type=F32).astype(BF16)
            for d in range(D):
                for r in range(D):
                    at = (d * D + r) * SUB
                    for g in range(lo, hi):
                        dense[buf, d * sub_rows + g * SUB:d * sub_rows + (g + 1) * SUB, r * LANES:(r + 1) * LANES] = part[
                            at:at + SUB, (g - lo) * LANES:(g - lo + 1) * LANES]

    def new_rows(slot, t, legs, bonds, buf, target):
        p = t // 2
        position = (t % 2) * sub_rows + iota((sub_rows, LANES), 0)
        row_live = position < limit_of(bonds[1], p)
        result = jnp.dot(dense[buf], right_x[slot], preferred_element_type=F32)
        for d in range(D):
            s = (p + legs[2][d]) % 2
            block = result[d * sub_rows:(d + 1) * sub_rows, :]
            chosen = jnp.where(s == 0, block[:, :LANES], block[:, LANES:])
            alive = row_live & (iota((sub_rows, LANES), 1) < limit_of(bonds[3], s))
            target[:, d * BLOCK:(d + 1) * BLOCK] = jnp.where(alive, chosen, 0.0).astype(BF16)[:, :BLOCK]

    def returned(t):
        return pltpu.make_async_remote_copy(
            src_ref=answer.at[t], dst_ref=out_ref.at[me],
            send_sem=send_sem.at[5, t], recv_sem=recv_sem.at[5, me],
            device_id={"blk": t}, device_id_type=MESH)

    second = 1 + lax.rem(me, last)
    third = 1 + lax.rem(second, last)

    @pl.when(worker)
    def _():
        for t in range(1, n_blk):
            here(1, t)
        boundary_ready(1, bonds_mine)
        mixed_rows(1, second, legs_mine, left_all[rows(second), :], 0)

        right_ready(1, legs_mine, bonds_mine)
        new_rows(1, second, legs_mine, bonds_mine, 0, answer.at[second])
        returned(second).start()
        mixed_rows(1, third, legs_mine, left_all[rows(third), :], 1)
        new_rows(1, third, legs_mine, bonds_mine, 1, answer.at[third])
        returned(third).start()

    @pl.when(worker)
    def _():
        here(1, 0)
        mixed_rows(1, 0, legs_mine, left_all[rows(0), :], 0)
        new_rows(1, 0, legs_mine, bonds_mine, 0, answer.at[0])
        returned(0).start()
        mixed_rows(1, me, legs_mine, left_all[rows(me), :], 1)
        new_rows(1, me, legs_mine, bonds_mine, 1, out_ref.at[me])

    boundary_ready(0, bonds_shared)
    own_shared.wait()
    mixed_rows(0, me, legs_shared, left_shared[...], 0)
    right_ready(0, legs_shared, bonds_shared)
    new_rows(0, me, legs_shared, bonds_shared, 0, out_ref.at[0])

    @pl.when(col == 0)
    def _():
        pass_beyond()

    for t in range(1, n_blk):
        @pl.when(me != t)
        def _():
            pltpu.make_async_remote_copy(
                src_ref=answer.at[t], dst_ref=out_ref.at[t],
                send_sem=send_sem.at[5, t], recv_sem=recv_sem.at[5, t],
                device_id={"blk": t}, device_id_type=MESH).wait_recv()
            for kind in kinds_to[t]:
                sent(kind, t).wait_send()

    beyond.wait_send()

    @pl.when(worker)
    def _():
        sent(3, 0).wait_send()
        sent(4, 0).wait_send()
        returned(0).wait_send()
        returned(second).wait_send()
        returned(third).wait_send()


def per_device(axis_sizes, boundary, row_tensor, left_proj, right_proj, leg_parity, bond_charges):
    col_dev, sub_rows, merged = boundary.shape
    n_blk = axis_sizes[1]
    padded = n_blk * sub_rows
    legs = leg_parity.transpose(1, 2, 0)
    bonds = bond_charges.transpose(1, 0)
    rows = row_tensor.transpose(1, 2, 3, 0, 4).reshape(D * D * D * col_dev, D)
    hbm = pl.BlockSpec(memory_space=pltpu.HBM)
    vmem = pl.BlockSpec(memory_space=pltpu.VMEM)
    return pl.pallas_call(
        functools.partial(kernel, axis_sizes),
        out_shape=pltpu.VMEM(boundary.shape, BF16),
        in_specs=[hbm] * 6,
        out_specs=vmem,
        scratch_shapes=[
            pltpu.VMEM(rows.shape, BF16),
            pltpu.SMEM(legs.shape, jnp.int32),
            pltpu.SMEM(bonds.shape, jnp.int32),
            pltpu.VMEM((2, padded, merged), BF16),
            pltpu.VMEM((padded, merged), BF16),
            pltpu.VMEM((sub_rows, merged), BF16),
            pltpu.VMEM((2, padded, merged), BF16),
            pltpu.VMEM((2, 2 * LANES, D * LANES), BF16),
            pltpu.VMEM((2, D * sub_rows, 2 * LANES), BF16),
            pltpu.VMEM((2, D * LANES, 2 * LANES), BF16),
            pltpu.VMEM((3, WIDE, WIDE), BF16),
            pltpu.VMEM((2, WIDE, (sub_rows // SUB) * LANES), BF16),
            pltpu.VMEM((2, D * sub_rows, D * LANES), BF16),
            pltpu.VMEM((n_blk, sub_rows, merged), BF16),
            pltpu.SemaphoreType.DMA((7, n_blk)),
            pltpu.SemaphoreType.DMA((7, n_blk)),
            pltpu.SemaphoreType.DMA((9,)),
            pltpu.SemaphoreType.REGULAR((2,)),
        ],
        compiler_params=pltpu.CompilerParams(collective_id=0, has_side_effects=True, vmem_limit_bytes=VMEM_BYTES),
    )(boundary, left_proj, right_proj, rows, legs, bonds)


def solution(mesh):
    axis_sizes = (mesh.shape["col"], mesh.shape["blk"])
    in_specs = (
        P(("grp", "col"), "blk", None),
        P(("grp", "col"), None, None, None, None),
        P(("grp", "col"), "blk", None),
        P(("grp", "col"), "blk", None),
        P("grp", None, None),
        P("grp", None),
    )
    out_specs = P(("grp", "col"), "blk", None)
    return jax.shard_map(
        functools.partial(per_device, axis_sizes), mesh=mesh, in_specs=in_specs, out_specs=out_specs, check_vma=False
    )
```

```python
import functools

import jax
import jax.numpy as jnp
from jax import lax
from jax.experimental import pallas as pl
from jax.experimental.pallas import tpu as pltpu
from jax.sharding import PartitionSpec as P

CHI = 128
BLOCK = 96
D = 6
LANES = 128
SUB = 16
PAIRS = D * D
WIDE = PAIRS * SUB
VMEM_BYTES = 55 * 1024 * 1024

MESH = pl.DeviceIdType.MESH
F32 = jnp.float32
BF16 = jnp.bfloat16


def ones_where(condition):
    return jnp.where(condition, 1.0, 0.0).astype(F32)


def iota(shape, dim):
    return lax.broadcasted_iota(jnp.int32, shape, dim)


def by_group(scalars, index, width):
    out = jnp.full(index.shape, scalars[0], jnp.int32)
    for i in range(1, len(scalars)):
        out = jnp.where(index >= i * width, scalars[i], out)
    return out


def limit_of(count, parity):
    return jnp.where(parity == 0, count, CHI - count)


def kernel(axis_sizes, bound_ref, left_ref, right_ref, row_hbm, leg_hbm, bond_hbm, out_ref,
           row_ref, leg_ref, bond_ref, bound_all, left_all, left_shared, right_all, bound_x, left_x, right_x, mix, mid, dense, answer,
           send_sem, recv_sem, local_sem, ready_sem):
    n_col, n_blk = axis_sizes
    col_dev, sub_rows, merged = bound_ref.shape
    me = lax.axis_index("blk")
    col = lax.axis_index("col")
    last = n_blk - 1
    col_before = lax.rem(col + n_col - 1, n_col)
    col_after = lax.rem(col + 1, n_col)
    cols = bond_hbm.shape[1]
    worker = me != 0

    barrier = pltpu.get_barrier_semaphore()
    pl.semaphore_signal(barrier, inc=1, device_id={"col": col_before, "blk": last}, device_id_type=MESH)

    @pl.when(worker)
    def _():
        for t in range(n_blk):
            @pl.when(me != t)
            def _():
                pl.semaphore_signal(barrier, inc=1, device_id={"blk": t}, device_id_type=MESH)

    def rows(t):
        return pl.ds(pl.multiple_of(t * sub_rows, SUB), sub_rows)

    targets = [bound_all.at[1], left_all, right_all.at[1], bound_all.at[0], right_all.at[0]]

    def source(kind, t):
        return (bound_ref.at[t], left_ref.at[t], right_ref.at[lax.rem(t + 1, col_dev)], bound_ref.at[0], right_ref.at[1])[kind]

    def own(kind):
        return pltpu.make_async_copy(source(kind, me), targets[kind].at[rows(me)], local_sem.at[kind])

    small = [pltpu.make_async_copy(a, b, local_sem.at[6 + i])
             for i, (a, b) in enumerate([(row_hbm, row_ref), (leg_hbm, leg_ref), (bond_hbm, bond_ref)])]
    for copy in small:
        copy.start()
    own(3).start()
    own(4).start()
    own_shared = pltpu.make_async_copy(left_ref.at[0], left_shared, local_sem.at[5])
    own_shared.start()

    @pl.when(worker)
    def _():
        own(0).start()
        own(1).start()

        @pl.when(me != last)
        def _():
            own(2).start()

    pl.semaphore_wait(barrier, jnp.where(me == 0, n_blk - 1, jnp.where(me == last, 2 * n_blk - 2, n_blk - 2)))

    def sent(kind, t):
        return pltpu.make_async_remote_copy(
            src_ref=source(kind, t), dst_ref=targets[kind].at[rows(me)],
            send_sem=send_sem.at[kind, t], recv_sem=recv_sem.at[kind, me],
            device_id={"blk": t}, device_id_type=MESH)

    def arrived(kind, t):
        return pltpu.make_async_remote_copy(
            src_ref=source(kind, 0), dst_ref=targets[kind].at[rows(t)],
            send_sem=send_sem.at[kind, t], recv_sem=recv_sem.at[kind, t],
            device_id={"blk": t}, device_id_type=MESH)

    beyond = pltpu.make_async_remote_copy(
        src_ref=right_ref.at[0], dst_ref=right_all.at[1, rows(me)],
        send_sem=send_sem.at[6, 0], recv_sem=recv_sem.at[2, me],
        device_id={"col": col_before, "blk": last}, device_id_type=MESH)

    @pl.when(me == 0)
    def _():
        for t in range(1, n_blk):
            pl.semaphore_signal(ready_sem.at[0], inc=1, device_id={"blk": t}, device_id_type=MESH)

    @pl.when(me == last)
    def _():
        for t in range(n_blk):
            pl.semaphore_signal(ready_sem.at[1], inc=1, device_id={"col": col_after, "blk": t}, device_id_type=MESH)

    far = n_blk // 2
    kinds_to = {t: ([0, 1, 2, 3, 4] if t != last else [0, 1, 3, 4]) for t in range(1, n_blk)}
    kinds_zero = {t: [0, 2, 1, 3, 4] for t in range(1, n_blk)}
    kinds_zero[far] = [0, 2, 1]
    kinds_zero[last] = [0, 3, 4, 1]
    order = [far] + [t for t in range(1, n_blk) if t != far]

    @pl.when(me == 0)
    def _():
        for place in range(5):
            for t in order:
                if place < len(kinds_zero[t]):
                    sent(kinds_zero[t][place], t).start()

    @pl.when(worker)
    def _():
        for kind in range(5):
            for t in order:
                if kind in kinds_to[t]:
                    @pl.when(me != t)
                    def _():
                        sent(kind, t).start()

    def passed_on(kind):
        return pltpu.make_async_remote_copy(
            src_ref=targets[kind].at[rows(0)], dst_ref=targets[kind].at[rows(0)],
            send_sem=send_sem.at[6, kind - 2], recv_sem=recv_sem.at[kind, 0],
            device_id={"blk": far}, device_id_type=MESH)

    for copy in small:
        copy.wait()

    triples = D * D * D
    group = iota((WIDE, triples), 0) // SUB
    member = iota((WIDE, triples), 1)
    repeat = ones_where((member >= group * D) & (member < group * D + D)).astype(BF16)
    pair = ones_where(iota((WIDE, LANES), 0) // SUB == iota((WIDE, LANES), 1)).astype(BF16)
    same = ones_where(iota((WIDE, WIDE), 0) % SUB == iota((WIDE, WIDE), 1) % SUB)
    spread = ones_where((iota((D, LANES), 1) - iota((D, LANES), 0)) % D == 0).astype(BF16)
    row = iota((triples, LANES), 0)
    lane = iota((triples, LANES), 1)
    d_row = row % D
    from_row = iota((triples, triples * col_dev), 0) * col_dev
    from_lane = iota((triples, triples * col_dev), 1)

    def legs_of(place):
        here = col * col_dev + place
        after = lax.rem(here + 1, cols)
        legs = [[leg_ref[i, j, here] for j in range(D)] for i in range(3)] + [[leg_ref[0, j, after] for j in range(D)]]
        return legs, (bond_ref[0, here], bond_ref[1, here], bond_ref[0, after], bond_ref[1, after])

    def build(place, legs, at):
        p0, p1, p2, pr = legs
        pick = ones_where(from_lane == from_row + place).astype(BF16)
        entries = jnp.dot(pick, row_ref[...], preferred_element_type=F32).astype(BF16)
        entries = jnp.dot(entries, spread, preferred_element_type=F32)
        legs_l = by_group(p0, row, D * D)
        legs_u = by_group(p1, (row // D) % D, 1)
        legs_d = by_group(p2, d_row, 1)
        legs_r = by_group(pr, lane % D, 1)
        keep = (d_row == lane // D) & ((legs_l + legs_u + legs_d + legs_r) % 2 == 0)
        sign = 1 - 2 * legs_l * legs_u
        q = (legs_d + legs_r) % 2
        signed = jnp.where(keep, sign * (1 - 2 * q * legs_d), 0).astype(F32)
        stretched = jnp.dot(repeat, (entries * signed).astype(BF16), preferred_element_type=F32).astype(BF16)
        full = lax.dot_general(pair, stretched, (((1,), (1,)), ((), ())), preferred_element_type=F32)
        mix[at] = (full * same).astype(BF16)

    legs_shared, bonds_shared = legs_of(0)
    legs_mine, bonds_mine = legs_of(me)
    build(0, legs_shared, 0)

    @pl.when(worker)
    def _():
        build(me, legs_mine, 1)

    gap = LANES - BLOCK
    lane_pad = jnp.zeros((sub_rows, gap), BF16)
    for slot in range(2):
        for p in range(2):
            bound_x[slot, p * LANES + BLOCK:(p + 1) * LANES, :] = jnp.zeros((gap, D * LANES), BF16)
        for r in range(D):
            right_x[slot, r * LANES + BLOCK:(r + 1) * LANES, :] = jnp.zeros((gap, 2 * LANES), BF16)

    @pl.when(worker)
    def _():
        pl.semaphore_wait(ready_sem.at[0], 1)
        sent(3, 0).start()
        sent(4, 0).start()

    def pass_beyond():
        pl.semaphore_wait(ready_sem.at[1], 1)
        beyond.start()

    @pl.when(col != 0)
    def _():
        pass_beyond()

    def widened(value, i):
        return jnp.concatenate([value[:, i * BLOCK:(i + 1) * BLOCK], lane_pad], axis=1)

    def here(kind, t):
        early = t == 0 and kind >= 3

        @pl.when((me != t) & (me != last) if early else me != t)
        def _():
            arrived(kind, t).wait_recv()

        @pl.when(me == t)
        def _():
            if kind == 2 and t == last:
                arrived(kind, t).wait_recv()
            else:
                own(kind).wait()

    def boundary_ready(slot, bonds):
        for t in reversed(range(n_blk)):
            here(0 if slot else 3, t)
            p, half = t // 2, t % 2
            live = ones_where(half * sub_rows + iota((sub_rows, LANES), 0) < limit_of(bonds[0], p)).astype(BF16)
            value = bound_all[slot, t * sub_rows:(t + 1) * sub_rows, :]
            at = p * LANES + half * sub_rows
            for u in range(D):
                bound_x[slot, at:at + sub_rows, u * LANES:(u + 1) * LANES] = widened(value, u) * live

    def right_ready(slot, legs, bonds):
        pr = legs[3]
        for t in reversed(range(n_blk)):
            here(2 if slot else 4, t)
            p, half = t // 2, t % 2
            position = half * sub_rows + iota((sub_rows, LANES), 0)
            live = ones_where(position < limit_of(bonds[2], p)).astype(BF16)
            value = right_all[slot, t * sub_rows:(t + 1) * sub_rows, :]
            for r in range(D):
                wide = widened(value, r) * live
                at = slice(r * LANES + half * sub_rows, r * LANES + (half + 1) * sub_rows)

                if p == 1:
                    right_x[slot, at, :LANES] = wide
                    right_x[slot, at, LANES:] = wide
                else:
                    right_x[slot, at, :LANES] = jnp.where(pr[r] == 0, wide, right_x[slot, at, :LANES])
                    right_x[slot, at, LANES:] = jnp.where(pr[r] == 0, right_x[slot, at, LANES:], wide)

    groups = sub_rows // SUB

    def mixed_rows(slot, units, legs, buf):
        tall = len(units) * sub_rows
        for i, (t, value) in enumerate(units):
            for leg in range(D):
                wide = widened(value, leg)
                odd = ((t // 2 + legs[0][leg]) % 2).astype(F32)
                at = slice(leg * tall + i * sub_rows, leg * tall + (i + 1) * sub_rows)
                left_x[buf, at, :LANES] = wide * (1.0 - odd).astype(BF16)
                left_x[buf, at, LANES:] = wide * odd.astype(BF16)
        count = len(units) * groups
        for n in range(D // 2):
            part = jnp.dot(left_x[buf, :D * tall], bound_x[slot, :, n * 2 * LANES:(n + 1) * 2 * LANES],
                           preferred_element_type=F32).astype(BF16)
            for leg in range(D):
                for v in range(2):
                    at = (leg * D + 2 * n + v) * SUB
                    for g in range(count):
                        mid[buf, at:at + SUB, g * LANES:(g + 1) * LANES] = part[
                            leg * tall + g * SUB:leg * tall + (g + 1) * SUB, v * LANES:(v + 1) * LANES]
        for lo in range(0, count, 2):
            hi = min(lo + 2, count)
            part = jnp.dot(mix[slot], mid[buf, :, lo * LANES:hi * LANES], preferred_element_type=F32).astype(BF16)
            for d in range(D):
                for r in range(D):
                    at = (d * D + r) * SUB
                    for g in range(lo, hi):
                        dense[buf, d * tall + g * SUB:d * tall + (g + 1) * SUB, r * LANES:(r + 1) * LANES] = part[
                            at:at + SUB, (g - lo) * LANES:(g - lo + 1) * LANES]

    def new_rows(slot, units, legs, bonds, buf):
        tall = len(units) * sub_rows
        result = jnp.dot(dense[buf, :D * tall], right_x[slot], preferred_element_type=F32)
        for i, (t, target) in enumerate(units):
            p = t // 2
            position = (t % 2) * sub_rows + iota((sub_rows, LANES), 0)
            row_live = position < limit_of(bonds[1], p)
            for d in range(D):
                s = (p + legs[2][d]) % 2
                at = d * tall + i * sub_rows
                block = result[at:at + sub_rows, :]
                chosen = jnp.where(s == 0, block[:, :LANES], block[:, LANES:]) * (1 - 2 * p * legs[2][d]).astype(F32)
                alive = row_live & (iota((sub_rows, LANES), 1) < limit_of(bonds[3], s))
                target[:, d * BLOCK:(d + 1) * BLOCK] = jnp.where(alive, chosen, 0.0).astype(BF16)[:, :BLOCK]

    def returned(t):
        return pltpu.make_async_remote_copy(
            src_ref=answer.at[t], dst_ref=out_ref.at[me],
            send_sem=send_sem.at[5, t], recv_sem=recv_sem.at[5, me],
            device_id={"blk": t}, device_id_type=MESH)

    second = 1 + lax.rem(me, last)
    third = 1 + lax.rem(second, last)

    @pl.when(worker)
    def _():
        for t in range(1, n_blk):
            here(1, t)
        boundary_ready(1, bonds_mine)
        mixed_rows(1, [(t, left_all[rows(t), :]) for t in (second, third)], legs_mine, 0)

    @pl.when(me == last)
    def _():
        for kind in (3, 4):
            arrived(kind, 0).wait_recv()
            passed_on(kind).start()

    @pl.when(worker)
    def _():
        right_ready(1, legs_mine, bonds_mine)
        new_rows(1, [(t, answer.at[t]) for t in (second, third)], legs_mine, bonds_mine, 0)
        returned(second).start()
        returned(third).start()
        here(1, 0)
        mixed_rows(1, [(0, left_all[rows(0), :]), (me, left_all[rows(me), :])], legs_mine, 1)
        new_rows(1, [(0, answer.at[0]), (me, out_ref.at[me])], legs_mine, bonds_mine, 1)
        returned(0).start()

    boundary_ready(0, bonds_shared)
    own_shared.wait()
    mixed_rows(0, [(me, left_shared[...])], legs_shared, 0)
    right_ready(0, legs_shared, bonds_shared)
    new_rows(0, [(me, out_ref.at[0])], legs_shared, bonds_shared, 0)

    @pl.when(col == 0)
    def _():
        pass_beyond()

    for t in range(1, n_blk):
        @pl.when(me != t)
        def _():
            pltpu.make_async_remote_copy(
                src_ref=answer.at[t], dst_ref=out_ref.at[t],
                send_sem=send_sem.at[5, t], recv_sem=recv_sem.at[5, t],
                device_id={"blk": t}, device_id_type=MESH).wait_recv()

    @pl.when(me == 0)
    def _():
        for t in order:
            for kind in kinds_zero[t]:
                sent(kind, t).wait_send()

    @pl.when(me == last)
    def _():
        passed_on(3).wait_send()
        passed_on(4).wait_send()

    beyond.wait_send()

    @pl.when(worker)
    def _():
        for t in order:
            @pl.when(me != t)
            def _():
                for kind in kinds_to[t]:
                    sent(kind, t).wait_send()

        sent(3, 0).wait_send()
        sent(4, 0).wait_send()
        returned(0).wait_send()
        returned(second).wait_send()
        returned(third).wait_send()


def per_device(axis_sizes, boundary, row_tensor, left_proj, right_proj, leg_parity, bond_charges):
    col_dev, sub_rows, merged = boundary.shape
    n_blk = axis_sizes[1]
    padded = n_blk * sub_rows
    legs = leg_parity.transpose(1, 2, 0)
    bonds = bond_charges.transpose(1, 0)
    rows = row_tensor.transpose(1, 2, 3, 0, 4).reshape(D * D * D * col_dev, D)
    hbm = pl.BlockSpec(memory_space=pltpu.HBM)
    vmem = pl.BlockSpec(memory_space=pltpu.VMEM)
    return pl.pallas_call(
        functools.partial(kernel, axis_sizes),
        out_shape=pltpu.VMEM(boundary.shape, BF16),
        in_specs=[hbm] * 6,
        out_specs=vmem,
        scratch_shapes=[
            pltpu.VMEM(rows.shape, BF16),
            pltpu.SMEM(legs.shape, jnp.int32),
            pltpu.SMEM(bonds.shape, jnp.int32),
            pltpu.VMEM((2, padded, merged), BF16),
            pltpu.VMEM((padded, merged), BF16),
            pltpu.VMEM((sub_rows, merged), BF16),
            pltpu.VMEM((2, padded, merged), BF16),
            pltpu.VMEM((2, 2 * LANES, D * LANES), BF16),
            pltpu.VMEM((2, 2 * D * sub_rows, 2 * LANES), BF16),
            pltpu.VMEM((2, D * LANES, 2 * LANES), BF16),
            pltpu.VMEM((2, WIDE, WIDE), BF16),
            pltpu.VMEM((2, WIDE, 2 * (sub_rows // SUB) * LANES), BF16),
            pltpu.VMEM((2, 2 * D * sub_rows, D * LANES), BF16),
            pltpu.VMEM((n_blk, sub_rows, merged), BF16),
            pltpu.SemaphoreType.DMA((7, n_blk)),
            pltpu.SemaphoreType.DMA((7, n_blk)),
            pltpu.SemaphoreType.DMA((9,)),
            pltpu.SemaphoreType.REGULAR((2,)),
        ],
        compiler_params=pltpu.CompilerParams(collective_id=0, has_side_effects=True, vmem_limit_bytes=VMEM_BYTES),
    )(boundary, left_proj, right_proj, rows, legs, bonds)


def solution(mesh):
    axis_sizes = (mesh.shape["col"], mesh.shape["blk"])
    in_specs = (
        P(("grp", "col"), "blk", None),
        P(("grp", "col"), None, None, None, None),
        P(("grp", "col"), "blk", None),
        P(("grp", "col"), "blk", None),
        P("grp", None, None),
        P("grp", None),
    )
    out_specs = P(("grp", "col"), "blk", None)
    return jax.shard_map(
        functools.partial(per_device, axis_sizes), mesh=mesh, in_specs=in_specs, out_specs=out_specs, check_vma=False
    )
```

```python
import functools

import jax
import jax.numpy as jnp
from jax import lax
from jax.experimental import pallas as pl
from jax.experimental.pallas import tpu as pltpu
from jax.sharding import PartitionSpec as P

CHI = 128
BLOCK = 96
D = 6
LANES = 128
SUB = 16
PAIRS = D * D
WIDE = PAIRS * SUB
VMEM_BYTES = 55 * 1024 * 1024

MESH = pl.DeviceIdType.MESH
F32 = jnp.float32
BF16 = jnp.bfloat16


def ones_where(condition):
    return jnp.where(condition, 1.0, 0.0).astype(F32)


def iota(shape, dim):
    return lax.broadcasted_iota(jnp.int32, shape, dim)


def by_group(scalars, index, width):
    out = jnp.full(index.shape, scalars[0], jnp.int32)
    for i in range(1, len(scalars)):
        out = jnp.where(index >= i * width, scalars[i], out)
    return out


def limit_of(count, parity):
    return jnp.where(parity == 0, count, CHI - count)


def kernel(axis_sizes, bound_ref, left_ref, right_ref, row_hbm, leg_hbm, bond_hbm, out_ref,
           row_ref, leg_ref, bond_ref, bond_rows, bound_all, left_all, left_shared, right_all, bound_x, left_x, right_x, mix, mid, dense, answer,
           send_sem, recv_sem, local_sem, ready_sem):
    n_col, n_blk = axis_sizes
    col_dev, sub_rows, merged = bound_ref.shape
    me = lax.axis_index("blk")
    col = lax.axis_index("col")
    last = n_blk - 1
    col_before = lax.rem(col + n_col - 1, n_col)
    col_after = lax.rem(col + 1, n_col)
    cols = bond_hbm.shape[1]
    worker = me != 0

    barrier = pltpu.get_barrier_semaphore()
    pl.semaphore_signal(barrier, inc=1, device_id={"col": col_before, "blk": last}, device_id_type=MESH)

    @pl.when(worker)
    def _():
        for t in range(n_blk):
            @pl.when(me != t)
            def _():
                pl.semaphore_signal(barrier, inc=1, device_id={"blk": t}, device_id_type=MESH)

    def rows(t):
        return pl.ds(pl.multiple_of(t * sub_rows, SUB), sub_rows)

    targets = [bound_all.at[1], left_all, right_all.at[1], bound_all.at[0], right_all.at[0]]

    def source(kind, t):
        return (bound_ref.at[t], left_ref.at[t], right_ref.at[lax.rem(t + 1, col_dev)], bound_ref.at[0], right_ref.at[1])[kind]

    def own(kind):
        return pltpu.make_async_copy(source(kind, me), targets[kind].at[rows(me)], local_sem.at[kind])

    small = [pltpu.make_async_copy(a, b, local_sem.at[6 + i])
             for i, (a, b) in enumerate([(row_hbm, row_ref), (leg_hbm, leg_ref), (bond_hbm, bond_ref), (right_ref.at[0], bond_rows)])]
    for copy in small:
        copy.start()
    own(3).start()
    own(4).start()
    own_shared = pltpu.make_async_copy(left_ref.at[0], left_shared, local_sem.at[5])
    own_shared.start()

    @pl.when(worker)
    def _():
        own(0).start()
        own(1).start()

        @pl.when(me != last)
        def _():
            own(2).start()

    pl.semaphore_wait(barrier, jnp.where(me == 0, n_blk - 1, jnp.where(me == last, 2 * n_blk - 2, n_blk - 2)))

    def sent(kind, t):
        return pltpu.make_async_remote_copy(
            src_ref=source(kind, t), dst_ref=targets[kind].at[rows(me)],
            send_sem=send_sem.at[kind, t], recv_sem=recv_sem.at[kind, me],
            device_id={"blk": t}, device_id_type=MESH)

    def arrived(kind, t):
        return pltpu.make_async_remote_copy(
            src_ref=source(kind, 0), dst_ref=targets[kind].at[rows(t)],
            send_sem=send_sem.at[kind, t], recv_sem=recv_sem.at[kind, t],
            device_id={"blk": t}, device_id_type=MESH)

    beyond = pltpu.make_async_remote_copy(
        src_ref=bond_rows, dst_ref=right_all.at[1, rows(me)],
        send_sem=send_sem.at[6, 0], recv_sem=recv_sem.at[2, me],
        device_id={"col": col_before, "blk": last}, device_id_type=MESH)

    @pl.when(me == 0)
    def _():
        for t in range(1, n_blk):
            pl.semaphore_signal(ready_sem.at[0], inc=1, device_id={"blk": t}, device_id_type=MESH)

    @pl.when(me == last)
    def _():
        for t in range(n_blk):
            pl.semaphore_signal(ready_sem.at[1], inc=1, device_id={"col": col_after, "blk": t}, device_id_type=MESH)

    far = n_blk // 2
    kinds_to = {t: ([0, 1, 2, 3, 4] if t != last else [0, 1, 3, 4]) for t in range(1, n_blk)}
    kinds_zero = {t: [0, 2, 1, 3, 4] for t in range(1, n_blk)}
    kinds_zero[far] = [0, 2, 1]
    kinds_zero[last] = [0, 3, 4, 1]
    order = [far] + [t for t in range(1, n_blk) if t != far]

    @pl.when(me == 0)
    def _():
        for place in range(5):
            for t in order:
                if place < len(kinds_zero[t]):
                    sent(kinds_zero[t][place], t).start()

    @pl.when(worker)
    def _():
        for kind in range(5):
            for t in order:
                if kind in kinds_to[t]:
                    @pl.when(me != t)
                    def _():
                        sent(kind, t).start()

    def passed_on(kind):
        return pltpu.make_async_remote_copy(
            src_ref=targets[kind].at[rows(0)], dst_ref=targets[kind].at[rows(0)],
            send_sem=send_sem.at[6, kind - 2], recv_sem=recv_sem.at[kind, 0],
            device_id={"blk": far}, device_id_type=MESH)

    for copy in small:
        copy.wait()

    triples = D * D * D
    group = iota((WIDE, triples), 0) // SUB
    member = iota((WIDE, triples), 1)
    repeat = ones_where((member >= group * D) & (member < group * D + D)).astype(BF16)
    pair = ones_where(iota((WIDE, LANES), 0) // SUB == iota((WIDE, LANES), 1)).astype(BF16)
    same = ones_where(iota((WIDE, WIDE), 0) % SUB == iota((WIDE, WIDE), 1) % SUB)
    spread = ones_where((iota((D, LANES), 1) - iota((D, LANES), 0)) % D == 0).astype(BF16)
    row = iota((triples, LANES), 0)
    lane = iota((triples, LANES), 1)
    d_row = row % D
    from_row = iota((triples, triples * col_dev), 0) * col_dev
    from_lane = iota((triples, triples * col_dev), 1)

    def legs_of(place):
        here = col * col_dev + place
        after = lax.rem(here + 1, cols)
        legs = [[leg_ref[i, j, here] for j in range(D)] for i in range(3)] + [[leg_ref[0, j, after] for j in range(D)]]
        return legs, (bond_ref[0, here], bond_ref[1, here], bond_ref[0, after], bond_ref[1, after])

    def build(place, legs, at):
        p0, p1, p2, pr = legs
        pick = ones_where(from_lane == from_row + place).astype(BF16)
        entries = jnp.dot(pick, row_ref[...], preferred_element_type=F32).astype(BF16)
        entries = jnp.dot(entries, spread, preferred_element_type=F32)
        legs_l = by_group(p0, row, D * D)
        legs_u = by_group(p1, (row // D) % D, 1)
        legs_d = by_group(p2, d_row, 1)
        legs_r = by_group(pr, lane % D, 1)
        keep = (d_row == lane // D) & ((legs_l + legs_u + legs_d + legs_r) % 2 == 0)
        sign = 1 - 2 * legs_l * legs_u
        q = (legs_d + legs_r) % 2
        signed = jnp.where(keep, sign * (1 - 2 * q * legs_d), 0).astype(F32)
        stretched = jnp.dot(repeat, (entries * signed).astype(BF16), preferred_element_type=F32).astype(BF16)
        full = lax.dot_general(pair, stretched, (((1,), (1,)), ((), ())), preferred_element_type=F32)
        mix[at] = (full * same).astype(BF16)

    legs_shared, bonds_shared = legs_of(0)
    legs_mine, bonds_mine = legs_of(me)
    build(0, legs_shared, 0)

    @pl.when(worker)
    def _():
        build(me, legs_mine, 1)

    gap = LANES - BLOCK
    lane_pad = jnp.zeros((sub_rows, gap), BF16)
    for slot in range(2):
        for p in range(2):
            bound_x[slot, p * LANES + BLOCK:(p + 1) * LANES, :] = jnp.zeros((gap, D * LANES), BF16)
        for r in range(D):
            right_x[slot, r * LANES + BLOCK:(r + 1) * LANES, :] = jnp.zeros((gap, 2 * LANES), BF16)

    @pl.when(worker)
    def _():
        pl.semaphore_wait(ready_sem.at[0], 1)
        sent(3, 0).start()
        sent(4, 0).start()

    def pass_beyond():
        pl.semaphore_wait(ready_sem.at[1], 1)
        beyond.start()

    @pl.when(col != 0)
    def _():
        pass_beyond()

    def widened(value, i):
        return jnp.concatenate([value[:, i * BLOCK:(i + 1) * BLOCK], lane_pad], axis=1)

    def here(kind, t):
        early = t == 0 and kind >= 3

        @pl.when((me != t) & (me != last) if early else me != t)
        def _():
            arrived(kind, t).wait_recv()

        @pl.when(me == t)
        def _():
            if kind == 2 and t == last:
                arrived(kind, t).wait_recv()
            else:
                own(kind).wait()

    def boundary_ready(slot, bonds):
        for t in reversed(range(n_blk)):
            here(0 if slot else 3, t)
            p, half = t // 2, t % 2
            live = ones_where(half * sub_rows + iota((sub_rows, LANES), 0) < limit_of(bonds[0], p)).astype(BF16)
            value = bound_all[slot, t * sub_rows:(t + 1) * sub_rows, :]
            at = p * LANES + half * sub_rows
            for u in range(D):
                bound_x[slot, at:at + sub_rows, u * LANES:(u + 1) * LANES] = widened(value, u) * live

    def right_ready(slot, legs, bonds):
        pr = legs[3]
        for t in reversed(range(n_blk)):
            here(2 if slot else 4, t)
            p, half = t // 2, t % 2
            position = half * sub_rows + iota((sub_rows, LANES), 0)
            live = ones_where(position < limit_of(bonds[2], p)).astype(BF16)
            value = right_all[slot, t * sub_rows:(t + 1) * sub_rows, :]
            for r in range(D):
                wide = widened(value, r) * live
                at = slice(r * LANES + half * sub_rows, r * LANES + (half + 1) * sub_rows)

                if p == 1:
                    right_x[slot, at, :LANES] = wide
                    right_x[slot, at, LANES:] = wide
                else:
                    right_x[slot, at, :LANES] = jnp.where(pr[r] == 0, wide, right_x[slot, at, :LANES])
                    right_x[slot, at, LANES:] = jnp.where(pr[r] == 0, right_x[slot, at, LANES:], wide)

    groups = sub_rows // SUB

    def mixed_rows(slot, units, legs, buf):
        tall = len(units) * sub_rows
        for i, (t, value) in enumerate(units):
            for leg in range(D):
                wide = widened(value, leg)
                odd = ((t // 2 + legs[0][leg]) % 2).astype(F32)
                at = slice(leg * tall + i * sub_rows, leg * tall + (i + 1) * sub_rows)
                left_x[buf, at, :LANES] = wide * (1.0 - odd).astype(BF16)
                left_x[buf, at, LANES:] = wide * odd.astype(BF16)
        count = len(units) * groups
        for n in range(D // 2):
            part = jnp.dot(left_x[buf, :D * tall], bound_x[slot, :, n * 2 * LANES:(n + 1) * 2 * LANES],
                           preferred_element_type=F32).astype(BF16)
            for leg in range(D):
                for v in range(2):
                    at = (leg * D + 2 * n + v) * SUB
                    for g in range(count):
                        mid[buf, at:at + SUB, g * LANES:(g + 1) * LANES] = part[
                            leg * tall + g * SUB:leg * tall + (g + 1) * SUB, v * LANES:(v + 1) * LANES]
        for lo in range(0, count, 2):
            hi = min(lo + 2, count)
            part = jnp.dot(mix[slot], mid[buf, :, lo * LANES:hi * LANES], preferred_element_type=F32).astype(BF16)
            for d in range(D):
                for r in range(D):
                    at = (d * D + r) * SUB
                    for g in range(lo, hi):
                        dense[buf, d * tall + g * SUB:d * tall + (g + 1) * SUB, r * LANES:(r + 1) * LANES] = part[
                            at:at + SUB, (g - lo) * LANES:(g - lo + 1) * LANES]

    def new_rows(slot, units, legs, bonds, buf):
        tall = len(units) * sub_rows
        result = jnp.dot(dense[buf, :D * tall], right_x[slot], preferred_element_type=F32)
        for i, (t, target) in enumerate(units):
            p = t // 2
            position = (t % 2) * sub_rows + iota((sub_rows, LANES), 0)
            row_live = position < limit_of(bonds[1], p)
            for d in range(D):
                s = (p + legs[2][d]) % 2
                at = d * tall + i * sub_rows
                block = result[at:at + sub_rows, :]
                chosen = jnp.where(s == 0, block[:, :LANES], block[:, LANES:]) * (1 - 2 * p * legs[2][d]).astype(F32)
                alive = row_live & (iota((sub_rows, LANES), 1) < limit_of(bonds[3], s))
                target[:, d * BLOCK:(d + 1) * BLOCK] = jnp.where(alive, chosen, 0.0).astype(BF16)[:, :BLOCK]

    def returned(t):
        return pltpu.make_async_remote_copy(
            src_ref=answer.at[t], dst_ref=out_ref.at[me],
            send_sem=send_sem.at[5, t], recv_sem=recv_sem.at[5, me],
            device_id={"blk": t}, device_id_type=MESH)

    second = 1 + lax.rem(me, last)
    third = 1 + lax.rem(second, last)

    @pl.when(worker)
    def _():
        for t in range(1, n_blk):
            here(1, t)
        boundary_ready(1, bonds_mine)
        mixed_rows(1, [(t, left_all[rows(t), :]) for t in (second, third)], legs_mine, 0)

    @pl.when(me == last)
    def _():
        for kind in (3, 4):
            arrived(kind, 0).wait_recv()
            passed_on(kind).start()

    @pl.when(worker)
    def _():
        right_ready(1, legs_mine, bonds_mine)
        new_rows(1, [(t, answer.at[t]) for t in (second, third)], legs_mine, bonds_mine, 0)
        returned(second).start()
        returned(third).start()

    @pl.when(worker)
    def _():
        here(1, 0)
        mixed_rows(1, [(0, left_all[rows(0), :])], legs_mine, 1)
        new_rows(1, [(0, answer.at[0])], legs_mine, bonds_mine, 1)
        returned(0).start()

    @pl.when(col == 0)
    def _():
        pass_beyond()

    @pl.when(worker)
    def _():
        mixed_rows(1, [(me, left_all[rows(me), :])], legs_mine, 0)
        new_rows(1, [(me, out_ref.at[me])], legs_mine, bonds_mine, 0)

    boundary_ready(0, bonds_shared)
    own_shared.wait()
    mixed_rows(0, [(me, left_shared[...])], legs_shared, 1)
    right_ready(0, legs_shared, bonds_shared)
    new_rows(0, [(me, out_ref.at[0])], legs_shared, bonds_shared, 1)

    for t in range(1, n_blk):
        @pl.when(me != t)
        def _():
            pltpu.make_async_remote_copy(
                src_ref=answer.at[t], dst_ref=out_ref.at[t],
                send_sem=send_sem.at[5, t], recv_sem=recv_sem.at[5, t],
                device_id={"blk": t}, device_id_type=MESH).wait_recv()

    @pl.when(me == 0)
    def _():
        for t in order:
            for kind in kinds_zero[t]:
                sent(kind, t).wait_send()

    @pl.when(me == last)
    def _():
        passed_on(3).wait_send()
        passed_on(4).wait_send()

    beyond.wait_send()

    @pl.when(worker)
    def _():
        for t in order:
            @pl.when(me != t)
            def _():
                for kind in kinds_to[t]:
                    sent(kind, t).wait_send()

        sent(3, 0).wait_send()
        sent(4, 0).wait_send()
        returned(0).wait_send()
        returned(second).wait_send()
        returned(third).wait_send()


def per_device(axis_sizes, boundary, row_tensor, left_proj, right_proj, leg_parity, bond_charges):
    col_dev, sub_rows, merged = boundary.shape
    n_blk = axis_sizes[1]
    padded = n_blk * sub_rows
    legs = leg_parity.transpose(1, 2, 0)
    bonds = bond_charges.transpose(1, 0)
    rows = row_tensor.transpose(1, 2, 3, 0, 4).reshape(D * D * D * col_dev, D)
    hbm = pl.BlockSpec(memory_space=pltpu.HBM)
    vmem = pl.BlockSpec(memory_space=pltpu.VMEM)
    return pl.pallas_call(
        functools.partial(kernel, axis_sizes),
        out_shape=pltpu.VMEM(boundary.shape, BF16),
        in_specs=[hbm] * 6,
        out_specs=vmem,
        scratch_shapes=[
            pltpu.VMEM(rows.shape, BF16),
            pltpu.SMEM(legs.shape, jnp.int32),
            pltpu.SMEM(bonds.shape, jnp.int32),
            pltpu.VMEM((sub_rows, merged), BF16),
            pltpu.VMEM((2, padded, merged), BF16),
            pltpu.VMEM((padded, merged), BF16),
            pltpu.VMEM((sub_rows, merged), BF16),
            pltpu.VMEM((2, padded, merged), BF16),
            pltpu.VMEM((2, 2 * LANES, D * LANES), BF16),
            pltpu.VMEM((2, 2 * D * sub_rows, 2 * LANES), BF16),
            pltpu.VMEM((2, D * LANES, 2 * LANES), BF16),
            pltpu.VMEM((2, WIDE, WIDE), BF16),
            pltpu.VMEM((2, WIDE, 2 * (sub_rows // SUB) * LANES), BF16),
            pltpu.VMEM((2, 2 * D * sub_rows, D * LANES), BF16),
            pltpu.VMEM((n_blk, sub_rows, merged), BF16),
            pltpu.SemaphoreType.DMA((7, n_blk)),
            pltpu.SemaphoreType.DMA((7, n_blk)),
            pltpu.SemaphoreType.DMA((10,)),
            pltpu.SemaphoreType.REGULAR((2,)),
        ],
        compiler_params=pltpu.CompilerParams(collective_id=0, has_side_effects=True, vmem_limit_bytes=VMEM_BYTES),
    )(boundary, left_proj, right_proj, rows, legs, bonds)


def solution(mesh):
    axis_sizes = (mesh.shape["col"], mesh.shape["blk"])
    in_specs = (
        P(("grp", "col"), "blk", None),
        P(("grp", "col"), None, None, None, None),
        P(("grp", "col"), "blk", None),
        P(("grp", "col"), "blk", None),
        P("grp", None, None),
        P("grp", None),
    )
    out_specs = P(("grp", "col"), "blk", None)
    return jax.shard_map(
        functools.partial(per_device, axis_sizes), mesh=mesh, in_specs=in_specs, out_specs=out_specs, check_vma=False
    )
```

```python
import functools

import jax
import jax.numpy as jnp
from jax import lax
from jax.experimental import pallas as pl
from jax.experimental.pallas import tpu as pltpu
from jax.sharding import PartitionSpec as P

CHI = 128
BLOCK = 96
D = 6
LANES = 128
SUB = 16
PAIRS = D * D
WIDE = PAIRS * SUB
VMEM_BYTES = 55 * 1024 * 1024

MESH = pl.DeviceIdType.MESH
F32 = jnp.float32
BF16 = jnp.bfloat16


def ones_where(condition):
    return jnp.where(condition, 1.0, 0.0).astype(F32)


def iota(shape, dim):
    return lax.broadcasted_iota(jnp.int32, shape, dim)


def by_group(scalars, index, width):
    out = jnp.full(index.shape, scalars[0], jnp.int32)
    for i in range(1, len(scalars)):
        out = jnp.where(index >= i * width, scalars[i], out)
    return out


def limit_of(count, parity):
    return jnp.where(parity == 0, count, CHI - count)


def kernel(axis_sizes, bound_ref, left_ref, right_ref, row_hbm, leg_hbm, bond_hbm, out_ref,
           row_ref, leg_ref, bond_ref, bond_rows, bound_all, left_all, left_shared, right_all, bound_x, left_x, right_x, mix, mid, dense, answer,
           send_sem, recv_sem, local_sem, ready_sem):
    n_col, n_blk = axis_sizes
    col_dev, sub_rows, merged = bound_ref.shape
    me = lax.axis_index("blk")
    col = lax.axis_index("col")
    last = n_blk - 1
    col_before = lax.rem(col + n_col - 1, n_col)
    col_after = lax.rem(col + 1, n_col)
    cols = bond_hbm.shape[1]
    worker = me != 0

    barrier = pltpu.get_barrier_semaphore()
    pl.semaphore_signal(barrier, inc=1, device_id={"col": col_before, "blk": last}, device_id_type=MESH)

    @pl.when(worker)
    def _():
        for t in range(n_blk):
            @pl.when(me != t)
            def _():
                pl.semaphore_signal(barrier, inc=1, device_id={"blk": t}, device_id_type=MESH)

    def rows(t):
        return pl.ds(pl.multiple_of(t * sub_rows, SUB), sub_rows)

    targets = [bound_all.at[1], left_all, right_all.at[1], bound_all.at[0], right_all.at[0]]

    def source(kind, t):
        return (bound_ref.at[t], left_ref.at[t], right_ref.at[lax.rem(t + 1, col_dev)], bound_ref.at[0], right_ref.at[1])[kind]

    def own(kind):
        return pltpu.make_async_copy(source(kind, me), targets[kind].at[rows(me)], local_sem.at[kind])

    small = [pltpu.make_async_copy(a, b, local_sem.at[6 + i])
             for i, (a, b) in enumerate([(row_hbm, row_ref), (leg_hbm, leg_ref), (bond_hbm, bond_ref), (right_ref.at[0], bond_rows)])]
    own_shared = pltpu.make_async_copy(left_ref.at[0], left_shared, local_sem.at[5])

    def fetch():
        for copy in small:
            copy.start()
        own(3).start()
        own(4).start()
        own_shared.start()

    @pl.when(worker)
    def _():
        fetch()
        own(0).start()
        own(1).start()

        @pl.when(me != last)
        def _():
            own(2).start()

    pl.semaphore_wait(barrier, jnp.where(me == 0, n_blk - 1, jnp.where(me == last, 2 * n_blk - 2, n_blk - 2)))

    def sent(kind, t):
        return pltpu.make_async_remote_copy(
            src_ref=source(kind, t), dst_ref=targets[kind].at[rows(me)],
            send_sem=send_sem.at[kind, t], recv_sem=recv_sem.at[kind, me],
            device_id={"blk": t}, device_id_type=MESH)

    def arrived(kind, t):
        return pltpu.make_async_remote_copy(
            src_ref=source(kind, 0), dst_ref=targets[kind].at[rows(t)],
            send_sem=send_sem.at[kind, t], recv_sem=recv_sem.at[kind, t],
            device_id={"blk": t}, device_id_type=MESH)

    beyond = pltpu.make_async_remote_copy(
        src_ref=bond_rows, dst_ref=right_all.at[1, rows(me)],
        send_sem=send_sem.at[6, 0], recv_sem=recv_sem.at[2, me],
        device_id={"col": col_before, "blk": last}, device_id_type=MESH)

    @pl.when(me == 0)
    def _():
        for t in range(1, n_blk):
            pl.semaphore_signal(ready_sem.at[0], inc=1, device_id={"blk": t}, device_id_type=MESH)

    @pl.when(me == last)
    def _():
        for t in range(n_blk):
            pl.semaphore_signal(ready_sem.at[1], inc=1, device_id={"col": col_after, "blk": t}, device_id_type=MESH)

    far = n_blk // 2
    kinds_to = {t: ([0, 1, 2, 3, 4] if t != last else [0, 1, 3, 4]) for t in range(1, n_blk)}
    kinds_zero = {t: [0, 2, 1, 3, 4] for t in range(1, n_blk)}
    kinds_zero[far] = [0, 2, 1]
    kinds_zero[last] = [0, 3, 4, 1]
    order = [far] + [t for t in range(1, n_blk) if t != far]

    @pl.when(me == 0)
    def _():
        for place in range(5):
            for t in order:
                if place < len(kinds_zero[t]):
                    sent(kinds_zero[t][place], t).start()
        fetch()

    @pl.when(worker)
    def _():
        for kind in range(5):
            for t in order:
                if kind in kinds_to[t]:
                    @pl.when(me != t)
                    def _():
                        sent(kind, t).start()

    def passed_on(kind):
        return pltpu.make_async_remote_copy(
            src_ref=targets[kind].at[rows(0)], dst_ref=targets[kind].at[rows(0)],
            send_sem=send_sem.at[6, kind - 2], recv_sem=recv_sem.at[kind, 0],
            device_id={"blk": far}, device_id_type=MESH)

    for copy in small:
        copy.wait()

    triples = D * D * D
    group = iota((WIDE, triples), 0) // SUB
    member = iota((WIDE, triples), 1)
    repeat = ones_where((member >= group * D) & (member < group * D + D)).astype(BF16)
    pair = ones_where(iota((WIDE, LANES), 0) // SUB == iota((WIDE, LANES), 1)).astype(BF16)
    same = ones_where(iota((WIDE, WIDE), 0) % SUB == iota((WIDE, WIDE), 1) % SUB)
    spread = ones_where((iota((D, LANES), 1) - iota((D, LANES), 0)) % D == 0).astype(BF16)
    row = iota((triples, LANES), 0)
    lane = iota((triples, LANES), 1)
    d_row = row % D
    from_row = iota((triples, triples * col_dev), 0) * col_dev
    from_lane = iota((triples, triples * col_dev), 1)

    def legs_of(place):
        here = col * col_dev + place
        after = lax.rem(here + 1, cols)
        legs = [[leg_ref[i, j, here] for j in range(D)] for i in range(3)] + [[leg_ref[0, j, after] for j in range(D)]]
        return legs, (bond_ref[0, here], bond_ref[1, here], bond_ref[0, after], bond_ref[1, after])

    def build(place, legs, at):
        p0, p1, p2, pr = legs
        pick = ones_where(from_lane == from_row + place).astype(BF16)
        entries = jnp.dot(pick, row_ref[...], preferred_element_type=F32).astype(BF16)
        entries = jnp.dot(entries, spread, preferred_element_type=F32)
        legs_l = by_group(p0, row, D * D)
        legs_u = by_group(p1, (row // D) % D, 1)
        legs_d = by_group(p2, d_row, 1)
        legs_r = by_group(pr, lane % D, 1)
        keep = (d_row == lane // D) & ((legs_l + legs_u + legs_d + legs_r) % 2 == 0)
        sign = 1 - 2 * legs_l * legs_u
        q = (legs_d + legs_r) % 2
        signed = jnp.where(keep, sign * (1 - 2 * q * legs_d), 0).astype(F32)
        stretched = jnp.dot(repeat, (entries * signed).astype(BF16), preferred_element_type=F32).astype(BF16)
        full = lax.dot_general(pair, stretched, (((1,), (1,)), ((), ())), preferred_element_type=F32)
        mix[at] = (full * same).astype(BF16)

    legs_shared, bonds_shared = legs_of(0)
    legs_mine, bonds_mine = legs_of(me)
    build(0, legs_shared, 0)

    @pl.when(worker)
    def _():
        build(me, legs_mine, 1)

    gap = LANES - BLOCK
    lane_pad = jnp.zeros((sub_rows, gap), BF16)
    for slot in range(2):
        for p in range(2):
            bound_x[slot, p * LANES + BLOCK:(p + 1) * LANES, :] = jnp.zeros((gap, D * LANES), BF16)
        for r in range(D):
            right_x[slot, r * LANES + BLOCK:(r + 1) * LANES, :] = jnp.zeros((gap, 2 * LANES), BF16)

    @pl.when(worker)
    def _():
        pl.semaphore_wait(ready_sem.at[0], 1)
        sent(3, 0).start()
        sent(4, 0).start()

    def pass_beyond():
        pl.semaphore_wait(ready_sem.at[1], 1)
        beyond.start()

    @pl.when(col != 0)
    def _():
        pass_beyond()

    def widened(value, i):
        return jnp.concatenate([value[:, i * BLOCK:(i + 1) * BLOCK], lane_pad], axis=1)

    def here(kind, t):
        early = t == 0 and kind >= 3

        @pl.when((me != t) & (me != last) if early else me != t)
        def _():
            arrived(kind, t).wait_recv()

        @pl.when(me == t)
        def _():
            if kind == 2 and t == last:
                arrived(kind, t).wait_recv()
            else:
                own(kind).wait()

    def boundary_ready(slot, bonds):
        for t in reversed(range(n_blk)):
            here(0 if slot else 3, t)
            p, half = t // 2, t % 2
            live = ones_where(half * sub_rows + iota((sub_rows, LANES), 0) < limit_of(bonds[0], p)).astype(BF16)
            value = bound_all[slot, t * sub_rows:(t + 1) * sub_rows, :]
            at = p * LANES + half * sub_rows
            for u in range(D):
                bound_x[slot, at:at + sub_rows, u * LANES:(u + 1) * LANES] = widened(value, u) * live

    def right_ready(slot, legs, bonds):
        pr = legs[3]
        for t in reversed(range(n_blk)):
            here(2 if slot else 4, t)
            p, half = t // 2, t % 2
            position = half * sub_rows + iota((sub_rows, LANES), 0)
            live = ones_where(position < limit_of(bonds[2], p)).astype(BF16)
            value = right_all[slot, t * sub_rows:(t + 1) * sub_rows, :]
            for r in range(D):
                wide = widened(value, r) * live
                at = slice(r * LANES + half * sub_rows, r * LANES + (half + 1) * sub_rows)

                if p == 1:
                    right_x[slot, at, :LANES] = wide
                    right_x[slot, at, LANES:] = wide
                else:
                    right_x[slot, at, :LANES] = jnp.where(pr[r] == 0, wide, right_x[slot, at, :LANES])
                    right_x[slot, at, LANES:] = jnp.where(pr[r] == 0, right_x[slot, at, LANES:], wide)

    groups = sub_rows // SUB

    def spread_left(units, legs, buf, first=0, count=None):
        tall = (count or len(units)) * sub_rows
        for i, (t, value) in enumerate(units, first):
            for leg in range(D):
                wide = widened(value, leg)
                odd = ((t // 2 + legs[0][leg]) % 2).astype(F32)
                at = slice(leg * tall + i * sub_rows, leg * tall + (i + 1) * sub_rows)
                left_x[buf, at, :LANES] = wide * (1.0 - odd).astype(BF16)
                left_x[buf, at, LANES:] = wide * odd.astype(BF16)

    def mixed_rows(slot, units, buf):
        tall = units * sub_rows
        count = units * groups
        for n in range(D // 2):
            part = jnp.dot(left_x[buf, :D * tall], bound_x[slot, :, n * 2 * LANES:(n + 1) * 2 * LANES],
                           preferred_element_type=F32).astype(BF16)
            for leg in range(D):
                for v in range(2):
                    at = (leg * D + 2 * n + v) * SUB
                    for g in range(count):
                        mid[buf, at:at + SUB, g * LANES:(g + 1) * LANES] = part[
                            leg * tall + g * SUB:leg * tall + (g + 1) * SUB, v * LANES:(v + 1) * LANES]
        for lo in range(0, count, 2):
            hi = min(lo + 2, count)
            part = jnp.dot(mix[slot], mid[buf, :, lo * LANES:hi * LANES], preferred_element_type=F32).astype(BF16)
            for d in range(D):
                for r in range(D):
                    at = (d * D + r) * SUB
                    for g in range(lo, hi):
                        dense[buf, d * tall + g * SUB:d * tall + (g + 1) * SUB, r * LANES:(r + 1) * LANES] = part[
                            at:at + SUB, (g - lo) * LANES:(g - lo + 1) * LANES]

    def new_rows(slot, units, legs, bonds, buf):
        tall = len(units) * sub_rows
        result = jnp.dot(dense[buf, :D * tall], right_x[slot], preferred_element_type=F32)
        for i, (t, target) in enumerate(units):
            p = t // 2
            position = (t % 2) * sub_rows + iota((sub_rows, LANES), 0)
            row_live = position < limit_of(bonds[1], p)
            for d in range(D):
                s = (p + legs[2][d]) % 2
                at = d * tall + i * sub_rows
                block = result[at:at + sub_rows, :]
                chosen = jnp.where(s == 0, block[:, :LANES], block[:, LANES:]) * (1 - 2 * p * legs[2][d]).astype(F32)
                alive = row_live & (iota((sub_rows, LANES), 1) < limit_of(bonds[3], s))
                target[:, d * BLOCK:(d + 1) * BLOCK] = jnp.where(alive, chosen, 0.0).astype(BF16)[:, :BLOCK]

    def returned(t):
        return pltpu.make_async_remote_copy(
            src_ref=answer.at[t], dst_ref=out_ref.at[me],
            send_sem=send_sem.at[5, t], recv_sem=recv_sem.at[5, me],
            device_id={"blk": t}, device_id_type=MESH)

    second = 1 + lax.rem(me, last)
    third = 1 + lax.rem(second, last)

    def pass_beyond_first():
        @pl.when(col == 0)
        def _():
            pass_beyond()

    own_shared.wait()
    spread_left([(me, left_shared[...])], legs_shared, 2)

    @pl.when(worker)
    def _():
        for t in range(1, n_blk):
            here(1, t)
        spread_left([(t, left_all[rows(t), :]) for t in (second, third)], legs_mine, 0)
        spread_left([(me, left_all[rows(me), :])], legs_mine, 1, 1, 2)
        boundary_ready(1, bonds_mine)
        mixed_rows(1, 2, 0)

    @pl.when(me == last)
    def _():
        for kind in (3, 4):
            arrived(kind, 0).wait_recv()
            passed_on(kind).start()

    @pl.when(worker)
    def _():
        right_ready(1, legs_mine, bonds_mine)
        new_rows(1, [(t, answer.at[t]) for t in (second, third)], legs_mine, bonds_mine, 0)
        returned(second).start()
        returned(third).start()

    @pl.when(worker)
    def _():
        here(1, 0)
        spread_left([(0, left_all[rows(0), :])], legs_mine, 1, 0, 2)
        mixed_rows(1, 2, 1)
        new_rows(1, [(0, answer.at[0]), (me, out_ref.at[me])], legs_mine, bonds_mine, 1)
        returned(0).start()
        pass_beyond_first()

    @pl.when(me == 0)
    def _():
        pass_beyond_first()

    boundary_ready(0, bonds_shared)
    mixed_rows(0, 1, 2)
    right_ready(0, legs_shared, bonds_shared)
    new_rows(0, [(me, out_ref.at[0])], legs_shared, bonds_shared, 2)

    for t in range(1, n_blk):
        @pl.when(me != t)
        def _():
            pltpu.make_async_remote_copy(
                src_ref=answer.at[t], dst_ref=out_ref.at[t],
                send_sem=send_sem.at[5, t], recv_sem=recv_sem.at[5, t],
                device_id={"blk": t}, device_id_type=MESH).wait_recv()

    @pl.when(me == 0)
    def _():
        for t in order:
            for kind in kinds_zero[t]:
                sent(kind, t).wait_send()

    @pl.when(me == last)
    def _():
        passed_on(3).wait_send()
        passed_on(4).wait_send()

    beyond.wait_send()

    @pl.when(worker)
    def _():
        for t in order:
            @pl.when(me != t)
            def _():
                for kind in kinds_to[t]:
                    sent(kind, t).wait_send()

        sent(3, 0).wait_send()
        sent(4, 0).wait_send()
        returned(0).wait_send()
        returned(second).wait_send()
        returned(third).wait_send()


def per_device(axis_sizes, boundary, row_tensor, left_proj, right_proj, leg_parity, bond_charges):
    col_dev, sub_rows, merged = boundary.shape
    n_blk = axis_sizes[1]
    padded = n_blk * sub_rows
    legs = leg_parity.transpose(1, 2, 0)
    bonds = bond_charges.transpose(1, 0)
    rows = row_tensor.transpose(1, 2, 3, 0, 4).reshape(D * D * D * col_dev, D)
    hbm = pl.BlockSpec(memory_space=pltpu.HBM)
    vmem = pl.BlockSpec(memory_space=pltpu.VMEM)
    return pl.pallas_call(
        functools.partial(kernel, axis_sizes),
        out_shape=pltpu.VMEM(boundary.shape, BF16),
        in_specs=[hbm] * 6,
        out_specs=vmem,
        scratch_shapes=[
            pltpu.VMEM(rows.shape, BF16),
            pltpu.SMEM(legs.shape, jnp.int32),
            pltpu.SMEM(bonds.shape, jnp.int32),
            pltpu.VMEM((sub_rows, merged), BF16),
            pltpu.VMEM((2, padded, merged), BF16),
            pltpu.VMEM((padded, merged), BF16),
            pltpu.VMEM((sub_rows, merged), BF16),
            pltpu.VMEM((2, padded, merged), BF16),
            pltpu.VMEM((2, 2 * LANES, D * LANES), BF16),
            pltpu.VMEM((3, 2 * D * sub_rows, 2 * LANES), BF16),
            pltpu.VMEM((2, D * LANES, 2 * LANES), BF16),
            pltpu.VMEM((2, WIDE, WIDE), BF16),
            pltpu.VMEM((3, WIDE, 2 * (sub_rows // SUB) * LANES), BF16),
            pltpu.VMEM((3, 2 * D * sub_rows, D * LANES), BF16),
            pltpu.VMEM((n_blk, sub_rows, merged), BF16),
            pltpu.SemaphoreType.DMA((7, n_blk)),
            pltpu.SemaphoreType.DMA((7, n_blk)),
            pltpu.SemaphoreType.DMA((10,)),
            pltpu.SemaphoreType.REGULAR((2,)),
        ],
        compiler_params=pltpu.CompilerParams(collective_id=0, has_side_effects=True, vmem_limit_bytes=VMEM_BYTES),
    )(boundary, left_proj, right_proj, rows, legs, bonds)


def solution(mesh):
    axis_sizes = (mesh.shape["col"], mesh.shape["blk"])
    in_specs = (
        P(("grp", "col"), "blk", None),
        P(("grp", "col"), None, None, None, None),
        P(("grp", "col"), "blk", None),
        P(("grp", "col"), "blk", None),
        P("grp", None, None),
        P("grp", None),
    )
    out_specs = P(("grp", "col"), "blk", None)
    return jax.shard_map(
        functools.partial(per_device, axis_sizes), mesh=mesh, in_specs=in_specs, out_specs=out_specs, check_vma=False
    )
```

```python
import functools

import jax
import jax.numpy as jnp
from jax import lax
from jax.experimental import pallas as pl
from jax.experimental.pallas import tpu as pltpu
from jax.sharding import PartitionSpec as P

CHI = 128
BLOCK = 96
D = 6
LANES = 128
SUB = 16
PAIRS = D * D
WIDE = PAIRS * SUB
VMEM_BYTES = 55 * 1024 * 1024

MESH = pl.DeviceIdType.MESH
F32 = jnp.float32
BF16 = jnp.bfloat16


def ones_where(condition):
    return jnp.where(condition, 1.0, 0.0).astype(F32)


def iota(shape, dim):
    return lax.broadcasted_iota(jnp.int32, shape, dim)


def by_group(scalars, index, width):
    out = jnp.full(index.shape, scalars[0], jnp.int32)
    for i in range(1, len(scalars)):
        out = jnp.where(index >= i * width, scalars[i], out)
    return out


def limit_of(count, parity):
    return jnp.where(parity == 0, count, CHI - count)


def kernel(axis_sizes, bound_ref, left_ref, right_ref, row_hbm, leg_hbm, bond_hbm, out_ref,
           row_ref, leg_ref, bond_ref, bond_rows, bound_all, left_all, left_shared, right_all, bound_x, left_x, right_x, mix, mid, dense, answer,
           send_sem, recv_sem, local_sem, ready_sem):
    n_col, n_blk = axis_sizes
    col_dev, sub_rows, merged = bound_ref.shape
    me = lax.axis_index("blk")
    col = lax.axis_index("col")
    last = n_blk - 1
    col_before = lax.rem(col + n_col - 1, n_col)
    col_after = lax.rem(col + 1, n_col)
    cols = bond_hbm.shape[1]
    worker = me != 0

    barrier = pltpu.get_barrier_semaphore()
    pl.semaphore_signal(barrier, inc=1, device_id={"col": col_before, "blk": last}, device_id_type=MESH)

    @pl.when(worker)
    def _():
        for t in range(n_blk):
            @pl.when(me != t)
            def _():
                pl.semaphore_signal(barrier, inc=1, device_id={"blk": t}, device_id_type=MESH)

    def rows(t):
        return pl.ds(pl.multiple_of(t * sub_rows, SUB), sub_rows)

    targets = [bound_all.at[1], left_all, right_all.at[1], bound_all.at[0], right_all.at[0]]

    def source(kind, t):
        return (bound_ref.at[t], left_ref.at[t], right_ref.at[lax.rem(t + 1, col_dev)], bound_ref.at[0], right_ref.at[1])[kind]

    def own(kind):
        return pltpu.make_async_copy(source(kind, me), targets[kind].at[rows(me)], local_sem.at[kind])

    small = [pltpu.make_async_copy(a, b, local_sem.at[6 + i])
             for i, (a, b) in enumerate([(row_hbm, row_ref), (leg_hbm, leg_ref), (bond_hbm, bond_ref), (right_ref.at[0], bond_rows)])]
    own_shared = pltpu.make_async_copy(left_ref.at[0], left_shared, local_sem.at[5])

    def fetch():
        for copy in small:
            copy.start()
        own(3).start()
        own(4).start()
        own_shared.start()

    @pl.when(worker)
    def _():
        fetch()
        own(0).start()
        own(1).start()

        @pl.when(me != last)
        def _():
            own(2).start()

    pl.semaphore_wait(barrier, jnp.where(me == 0, n_blk - 1, jnp.where(me == last, 2 * n_blk - 2, n_blk - 2)))

    def sent(kind, t):
        return pltpu.make_async_remote_copy(
            src_ref=source(kind, t), dst_ref=targets[kind].at[rows(me)],
            send_sem=send_sem.at[kind, t], recv_sem=recv_sem.at[kind, me],
            device_id={"blk": t}, device_id_type=MESH)

    def arrived(kind, t):
        return pltpu.make_async_remote_copy(
            src_ref=source(kind, 0), dst_ref=targets[kind].at[rows(t)],
            send_sem=send_sem.at[kind, t], recv_sem=recv_sem.at[kind, t],
            device_id={"blk": t}, device_id_type=MESH)

    beyond = pltpu.make_async_remote_copy(
        src_ref=bond_rows, dst_ref=right_all.at[1, rows(me)],
        send_sem=send_sem.at[6, 0], recv_sem=recv_sem.at[2, me],
        device_id={"col": col_before, "blk": last}, device_id_type=MESH)

    @pl.when(me == 0)
    def _():
        for t in range(1, n_blk):
            pl.semaphore_signal(ready_sem.at[0], inc=1, device_id={"blk": t}, device_id_type=MESH)

    @pl.when(me == last)
    def _():
        for t in range(n_blk):
            pl.semaphore_signal(ready_sem.at[1], inc=1, device_id={"col": col_after, "blk": t}, device_id_type=MESH)

    far = n_blk // 2
    kinds_to = {t: ([0, 1, 2, 3, 4] if t != last else [0, 1, 3, 4]) for t in range(1, n_blk)}
    kinds_zero = {t: [0, 2, 1, 3, 4] for t in range(1, n_blk)}
    kinds_zero[far] = [0, 2, 1]
    kinds_zero[last] = [0, 3, 4, 1]
    order = [far] + [t for t in range(1, n_blk) if t != far]

    @pl.when(me == 0)
    def _():
        for place in range(5):
            for t in order:
                if place < len(kinds_zero[t]):
                    sent(kinds_zero[t][place], t).start()
        fetch()

    @pl.when(worker)
    def _():
        for kind in range(5):
            for t in order:
                if kind in kinds_to[t]:
                    @pl.when(me != t)
                    def _():
                        sent(kind, t).start()

    def passed_on(kind):
        return pltpu.make_async_remote_copy(
            src_ref=targets[kind].at[rows(0)], dst_ref=targets[kind].at[rows(0)],
            send_sem=send_sem.at[6, kind - 2], recv_sem=recv_sem.at[kind, 0],
            device_id={"blk": far}, device_id_type=MESH)

    for copy in small:
        copy.wait()

    triples = D * D * D
    group = iota((WIDE, triples), 0) // SUB
    member = iota((WIDE, triples), 1)
    repeat = ones_where((member >= group * D) & (member < group * D + D)).astype(BF16)
    pair = ones_where(iota((WIDE, LANES), 0) // SUB == iota((WIDE, LANES), 1)).astype(BF16)
    same = ones_where(iota((WIDE, WIDE), 0) % SUB == iota((WIDE, WIDE), 1) % SUB)
    spread = ones_where((iota((D, LANES), 1) - iota((D, LANES), 0)) % D == 0).astype(BF16)
    row = iota((triples, LANES), 0)
    lane = iota((triples, LANES), 1)
    d_row = row % D
    from_row = iota((triples, triples * col_dev), 0) * col_dev
    from_lane = iota((triples, triples * col_dev), 1)

    def legs_of(place):
        here = col * col_dev + place
        after = lax.rem(here + 1, cols)
        legs = [[leg_ref[i, j, here] for j in range(D)] for i in range(3)] + [[leg_ref[0, j, after] for j in range(D)]]
        return legs, (bond_ref[0, here], bond_ref[1, here], bond_ref[0, after], bond_ref[1, after])

    def build(place, legs, at):
        p0, p1, p2, pr = legs
        pick = ones_where(from_lane == from_row + place).astype(BF16)
        entries = jnp.dot(pick, row_ref[...], preferred_element_type=F32).astype(BF16)
        entries = jnp.dot(entries, spread, preferred_element_type=F32)
        legs_l = by_group(p0, row, D * D)
        legs_u = by_group(p1, (row // D) % D, 1)
        legs_d = by_group(p2, d_row, 1)
        legs_r = by_group(pr, lane % D, 1)
        keep = (d_row == lane // D) & ((legs_l + legs_u + legs_d + legs_r) % 2 == 0)
        sign = 1 - 2 * legs_l * legs_u
        q = (legs_d + legs_r) % 2
        signed = jnp.where(keep, sign * (1 - 2 * q * legs_d), 0).astype(F32)
        stretched = jnp.dot(repeat, (entries * signed).astype(BF16), preferred_element_type=F32).astype(BF16)
        full = lax.dot_general(pair, stretched, (((1,), (1,)), ((), ())), preferred_element_type=F32)
        mix[at] = (full * same).astype(BF16)

    legs_shared, bonds_shared = legs_of(0)
    legs_mine, bonds_mine = legs_of(me)
    build(0, legs_shared, 0)

    @pl.when(worker)
    def _():
        build(me, legs_mine, 1)

    gap = LANES - BLOCK
    lane_pad = jnp.zeros((sub_rows, gap), BF16)
    for slot in range(2):
        for p in range(2):
            bound_x[slot, p * LANES + BLOCK:(p + 1) * LANES, :] = jnp.zeros((gap, D * LANES), BF16)
        for r in range(D):
            right_x[slot, r * LANES + BLOCK:(r + 1) * LANES, :] = jnp.zeros((gap, 2 * LANES), BF16)

    @pl.when(worker)
    def _():
        pl.semaphore_wait(ready_sem.at[0], 1)
        sent(3, 0).start()
        sent(4, 0).start()

    def pass_beyond():
        pl.semaphore_wait(ready_sem.at[1], 1)
        beyond.start()

    @pl.when(col != 0)
    def _():
        pass_beyond()

    def widened(value, i):
        return jnp.concatenate([value[:, i * BLOCK:(i + 1) * BLOCK], lane_pad], axis=1)

    def here(kind, t):
        early = t == 0 and kind >= 3

        @pl.when((me != t) & (me != last) if early else me != t)
        def _():
            arrived(kind, t).wait_recv()

        @pl.when(me == t)
        def _():
            if kind == 2 and t == last:
                arrived(kind, t).wait_recv()
            else:
                own(kind).wait()

    def boundary_ready(slot, bonds, places):
        for t in places:
            here(0 if slot else 3, t)
            p, half = t // 2, t % 2
            live = ones_where(half * sub_rows + iota((sub_rows, LANES), 0) < limit_of(bonds[0], p)).astype(BF16)
            value = bound_all[slot, t * sub_rows:(t + 1) * sub_rows, :]
            at = p * LANES + half * sub_rows
            for u in range(D):
                bound_x[slot, at:at + sub_rows, u * LANES:(u + 1) * LANES] = widened(value, u) * live

    def right_ready(slot, legs, bonds, places):
        pr = legs[3]
        for t in places:
            here(2 if slot else 4, t)
            p, half = t // 2, t % 2
            position = half * sub_rows + iota((sub_rows, LANES), 0)
            live = ones_where(position < limit_of(bonds[2], p)).astype(BF16)
            value = right_all[slot, t * sub_rows:(t + 1) * sub_rows, :]
            for r in range(D):
                wide = widened(value, r) * live
                at = slice(r * LANES + half * sub_rows, r * LANES + (half + 1) * sub_rows)

                if p == 1:
                    right_x[slot, at, :LANES] = wide
                    right_x[slot, at, LANES:] = wide
                else:
                    right_x[slot, at, :LANES] = jnp.where(pr[r] == 0, wide, right_x[slot, at, :LANES])
                    right_x[slot, at, LANES:] = jnp.where(pr[r] == 0, right_x[slot, at, LANES:], wide)

    groups = sub_rows // SUB

    def spread_left(units, legs, buf, first=0, count=None):
        tall = (count or len(units)) * sub_rows
        for i, (t, value) in enumerate(units, first):
            for leg in range(D):
                wide = widened(value, leg)
                odd = ((t // 2 + legs[0][leg]) % 2).astype(F32)
                at = slice(leg * tall + i * sub_rows, leg * tall + (i + 1) * sub_rows)
                left_x[buf, at, :LANES] = wide * (1.0 - odd).astype(BF16)
                left_x[buf, at, LANES:] = wide * odd.astype(BF16)

    def mixed_rows(slot, units, buf):
        tall = units * sub_rows
        count = units * groups
        for n in range(D // 2):
            part = jnp.dot(left_x[buf, :D * tall], bound_x[slot, :, n * 2 * LANES:(n + 1) * 2 * LANES],
                           preferred_element_type=F32).astype(BF16)
            for leg in range(D):
                for v in range(2):
                    at = (leg * D + 2 * n + v) * SUB
                    for g in range(count):
                        mid[buf, at:at + SUB, g * LANES:(g + 1) * LANES] = part[
                            leg * tall + g * SUB:leg * tall + (g + 1) * SUB, v * LANES:(v + 1) * LANES]
        for lo in range(0, count, 2):
            hi = min(lo + 2, count)
            part = jnp.dot(mix[slot], mid[buf, :, lo * LANES:hi * LANES], preferred_element_type=F32).astype(BF16)
            for d in range(D):
                for r in range(D):
                    at = (d * D + r) * SUB
                    for g in range(lo, hi):
                        dense[buf, d * tall + g * SUB:d * tall + (g + 1) * SUB, r * LANES:(r + 1) * LANES] = part[
                            at:at + SUB, (g - lo) * LANES:(g - lo + 1) * LANES]

    def new_rows(slot, units, legs, bonds, buf):
        tall = len(units) * sub_rows
        result = jnp.dot(dense[buf, :D * tall], right_x[slot], preferred_element_type=F32)
        for i, (t, target) in enumerate(units):
            p = t // 2
            position = (t % 2) * sub_rows + iota((sub_rows, LANES), 0)
            row_live = position < limit_of(bonds[1], p)
            for d in range(D):
                s = (p + legs[2][d]) % 2
                at = d * tall + i * sub_rows
                block = result[at:at + sub_rows, :]
                chosen = jnp.where(s == 0, block[:, :LANES], block[:, LANES:]) * (1 - 2 * p * legs[2][d]).astype(F32)
                alive = row_live & (iota((sub_rows, LANES), 1) < limit_of(bonds[3], s))
                target[:, d * BLOCK:(d + 1) * BLOCK] = jnp.where(alive, chosen, 0.0).astype(BF16)[:, :BLOCK]

    def returned(t):
        return pltpu.make_async_remote_copy(
            src_ref=answer.at[t], dst_ref=out_ref.at[me],
            send_sem=send_sem.at[5, t], recv_sem=recv_sem.at[5, me],
            device_id={"blk": t}, device_id_type=MESH)

    everyone = list(reversed(range(n_blk)))
    second = 1 + lax.rem(me, last)
    third = 1 + lax.rem(second, last)

    def pass_beyond_first():
        @pl.when(col == 0)
        def _():
            pass_beyond()

    own_shared.wait()
    spread_left([(me, left_shared[...])], legs_shared, 2)

    @pl.when(worker)
    def _():
        for t in range(1, n_blk):
            here(1, t)
        spread_left([(t, left_all[rows(t), :]) for t in (second, third)], legs_mine, 0)
        spread_left([(me, left_all[rows(me), :])], legs_mine, 1, 1, 2)
        boundary_ready(1, bonds_mine, everyone)
        mixed_rows(1, 2, 0)

    @pl.when(me == last)
    def _():
        for kind in (3, 4):
            arrived(kind, 0).wait_recv()
            passed_on(kind).start()

    @pl.when(worker)
    def _():
        right_ready(1, legs_mine, bonds_mine, everyone)
        new_rows(1, [(t, answer.at[t]) for t in (second, third)], legs_mine, bonds_mine, 0)
        returned(second).start()
        returned(third).start()

    boundary_ready(0, bonds_shared, everyone[:-1])
    right_ready(0, legs_shared, bonds_shared, everyone[:-1])

    @pl.when(worker)
    def _():
        here(1, 0)
        spread_left([(0, left_all[rows(0), :])], legs_mine, 1, 0, 2)
        mixed_rows(1, 2, 1)
        new_rows(1, [(0, answer.at[0]), (me, out_ref.at[me])], legs_mine, bonds_mine, 1)
        returned(0).start()
        pass_beyond_first()

    @pl.when(me == 0)
    def _():
        pass_beyond_first()

    boundary_ready(0, bonds_shared, everyone[-1:])
    mixed_rows(0, 1, 2)
    right_ready(0, legs_shared, bonds_shared, everyone[-1:])
    new_rows(0, [(me, out_ref.at[0])], legs_shared, bonds_shared, 2)

    for t in range(1, n_blk):
        @pl.when(me != t)
        def _():
            pltpu.make_async_remote_copy(
                src_ref=answer.at[t], dst_ref=out_ref.at[t],
                send_sem=send_sem.at[5, t], recv_sem=recv_sem.at[5, t],
                device_id={"blk": t}, device_id_type=MESH).wait_recv()

    @pl.when(me == 0)
    def _():
        for t in order:
            for kind in kinds_zero[t]:
                sent(kind, t).wait_send()

    @pl.when(me == last)
    def _():
        passed_on(3).wait_send()
        passed_on(4).wait_send()

    beyond.wait_send()

    @pl.when(worker)
    def _():
        for t in order:
            @pl.when(me != t)
            def _():
                for kind in kinds_to[t]:
                    sent(kind, t).wait_send()

        sent(3, 0).wait_send()
        sent(4, 0).wait_send()
        returned(0).wait_send()
        returned(second).wait_send()
        returned(third).wait_send()


def per_device(axis_sizes, boundary, row_tensor, left_proj, right_proj, leg_parity, bond_charges):
    col_dev, sub_rows, merged = boundary.shape
    n_blk = axis_sizes[1]
    padded = n_blk * sub_rows
    legs = leg_parity.transpose(1, 2, 0)
    bonds = bond_charges.transpose(1, 0)
    rows = row_tensor.transpose(1, 2, 3, 0, 4).reshape(D * D * D * col_dev, D)
    hbm = pl.BlockSpec(memory_space=pltpu.HBM)
    vmem = pl.BlockSpec(memory_space=pltpu.VMEM)
    return pl.pallas_call(
        functools.partial(kernel, axis_sizes),
        out_shape=pltpu.VMEM(boundary.shape, BF16),
        in_specs=[hbm] * 6,
        out_specs=vmem,
        scratch_shapes=[
            pltpu.VMEM(rows.shape, BF16),
            pltpu.SMEM(legs.shape, jnp.int32),
            pltpu.SMEM(bonds.shape, jnp.int32),
            pltpu.VMEM((sub_rows, merged), BF16),
            pltpu.VMEM((2, padded, merged), BF16),
            pltpu.VMEM((padded, merged), BF16),
            pltpu.VMEM((sub_rows, merged), BF16),
            pltpu.VMEM((2, padded, merged), BF16),
            pltpu.VMEM((2, 2 * LANES, D * LANES), BF16),
            pltpu.VMEM((3, 2 * D * sub_rows, 2 * LANES), BF16),
            pltpu.VMEM((2, D * LANES, 2 * LANES), BF16),
            pltpu.VMEM((2, WIDE, WIDE), BF16),
            pltpu.VMEM((3, WIDE, 2 * (sub_rows // SUB) * LANES), BF16),
            pltpu.VMEM((3, 2 * D * sub_rows, D * LANES), BF16),
            pltpu.VMEM((n_blk, sub_rows, merged), BF16),
            pltpu.SemaphoreType.DMA((7, n_blk)),
            pltpu.SemaphoreType.DMA((7, n_blk)),
            pltpu.SemaphoreType.DMA((10,)),
            pltpu.SemaphoreType.REGULAR((2,)),
        ],
        compiler_params=pltpu.CompilerParams(collective_id=0, has_side_effects=True, vmem_limit_bytes=VMEM_BYTES),
    )(boundary, left_proj, right_proj, rows, legs, bonds)


def solution(mesh):
    axis_sizes = (mesh.shape["col"], mesh.shape["blk"])
    in_specs = (
        P(("grp", "col"), "blk", None),
        P(("grp", "col"), None, None, None, None),
        P(("grp", "col"), "blk", None),
        P(("grp", "col"), "blk", None),
        P("grp", None, None),
        P("grp", None),
    )
    out_specs = P(("grp", "col"), "blk", None)
    return jax.shard_map(
        functools.partial(per_device, axis_sizes), mesh=mesh, in_specs=in_specs, out_specs=out_specs, check_vma=False
    )
```
